256 devices in a mesh: section: 8 (over z_hi, core), expert: 32 (over z_lo, x, y).
Axes of the slice: x: 4, y: 4, z: 8 (z_hi: 4, z_lo: 2; z = z_hi * 2 + z_lo), core: 2. Of those that a mesh axis runs over, the one named last changes fastest.
Arguments:
- act_in: bfloat16 [8, 4096, 7168], P('section', 'expert'), may hold values from -6 to 6
- cotangent: bfloat16 [8, 4096, 7168], P('section', 'expert'), may hold values from -6 to 6
- fwd_ids: int32 [8, 4096, 8], P('section', 'expert'), may hold values from 0 to 255, as said below
- fwd_gates: float32 [8, 4096, 8], P('section', 'expert'), may hold values from 0.05 to 0.8
- bwd_ids: int32 [8, 4096, 8], P('section', 'expert'), may hold values from 0 to 255, as said below
- bwd_gates: float32 [8, 4096, 8], P('section', 'expert'), may hold values from 0.05 to 0.8
- gate_w: bfloat16 [8, 7168, 4096], P('section', None, 'expert'), may hold values from -0.0625 to 0.0625
- up_w: bfloat16 [8, 7168, 4096], P('section', None, 'expert'), may hold values from -0.0625 to 0.0625
- down_w: bfloat16 [8, 4096, 7168], P('section', 'expert'), may hold values from -0.125 to 0.125
- gate_pre: bfloat16 [8, 320, 4096], P('section', None, 'expert'), may hold values from -6 to 6
- up_pre: bfloat16 [8, 320, 4096], P('section', None, 'expert'), may hold values from -6 to 6
Outputs:
- next_act: bfloat16 [8, 4096, 7168], P('section', 'expert')
- prev_grad: bfloat16 [8, 4096, 7168], P('section', 'expert')
- gate_grad: float32 [8, 4096, 8], P('section', 'expert')
The draws below stay inside these ranges and needn't reach their ends.
Inputs may be any that keep to these rules, and one draw needn't show every extreme that they name: `fwd_ids`: the 8 ids of a row differ. In each aligned block of 128 rows (the rows of one device) each id below 2 is named by at most 10 rows; in every section one such id is named by exactly 10 rows in every block. `bwd_ids`: as for fwd_ids.
All inputs are finite; a program needn't handle non-finite values.
Results may differ from the reference program's by a relative error of at most 0.012.
Values may be sent and summed in bfloat16 or wider, within the bound.
A program may use at most 128 MiB of HBM per device.

```python
import math
import jax
import jax.numpy as jnp
from jax import lax

D = 7168
FF = 2048
ROUTED = 256
TOP = 8
TOK_DEV = 128
CAP = 10
SLICES = 16
FF_DEV = 128
EXPERTS = 2
SECTIONS = 8
TOKENS = 4096
SLOTS = 320


def route_draw(key):
    blocks = SECTIONS * (TOKENS // TOK_DEV)
    keys = [jax.random.fold_in(key, offset) for offset in range(5)]
    counts = jax.random.randint(keys[0], (blocks, EXPERTS), CAP // 2, CAP + 1)
    fullest = jax.random.randint(keys[1], (SECTIONS,), 0, EXPERTS)
    fullest_block = jnp.repeat(fullest, TOKENS // TOK_DEV)
    counts = jnp.where(jnp.arange(EXPERTS)[None, :] == fullest_block[:, None], CAP, counts)
    scores = jax.random.randint(keys[2], (blocks, EXPERTS, TOK_DEV), 0, 2 ** 20) * TOK_DEV + jnp.arange(TOK_DEV)
    order = jnp.argsort(jnp.argsort(scores, axis=-1), axis=-1)
    chosen = order < counts[:, :, None]
    others = jax.random.randint(keys[3], (blocks, TOK_DEV, ROUTED - EXPERTS), 0, 2 ** 20) * ROUTED + jnp.arange(ROUTED - EXPERTS)
    unused, picks = lax.top_k(others, TOP)
    ids = picks + EXPERTS
    slot_scores = jax.random.randint(keys[4], (blocks, TOK_DEV, TOP), 0, 2 ** 20) * TOP + jnp.arange(TOP)
    unused_two, places = lax.top_k(slot_scores, TOP)
    slot_iota = jnp.arange(TOP)
    for expert in range(EXPERTS):
        target = places[:, :, expert:expert + 1]
        put_here = (slot_iota[None, None, :] == target) & chosen[:, expert, :, None]
        ids = jnp.where(put_here, expert, ids)
    return ids.reshape(SECTIONS, TOKENS, TOP).astype(jnp.int32)


def draw_fwd_ids(key, part):
    return route_draw(jax.random.fold_in(key, 11))


def draw_bwd_ids(key, part):
    return route_draw(jax.random.fold_in(key, 23))


def block_scale(key, extent, pieces, least, high):
    def one(dim, shards_of):
        draws = jax.random.uniform(jax.random.fold_in(jax.random.fold_in(key, 6), dim), (shards_of,), jnp.float32, least / len(pieces), high / len(pieces))
        return jnp.repeat(jnp.exp(draws), extent[dim] // shards_of).reshape((-1,) + (1,) * (len(extent) - dim - 1))

    level = one(*pieces[0])
    for cut in pieces[1:]:
        level = level * one(*cut)
    return level


def scatter_about(key, shape, width, reach, shards=(), held_as=jnp.bfloat16):
    values = width * jax.random.normal(key, shape, jnp.float32)
    if shards:
        values = values * block_scale(key, shape, shards, -0.22, 0.18)
    return jnp.clip(values, -reach, reach).astype(held_as)


def setup_inputs(seed: int = 0) -> dict:
    streams_of = jax.random.split(jax.random.key(seed), 12)
    return {
        "act_in": scatter_about(streams_of[0], (SECTIONS, TOKENS, D), 1.0, 6.0, ((0, 8), (1, 32))),
        "cotangent": scatter_about(streams_of[1], (SECTIONS, TOKENS, D), 1.0, 6.0, ((0, 8), (1, 32))),
        "fwd_ids": draw_fwd_ids(jax.random.fold_in(streams_of[11], 71), 0),
        "fwd_gates": jnp.clip(jnp.exp(math.log(0.8) - 2.7725887 * jax.random.uniform(streams_of[3], (SECTIONS, TOKENS, TOP), jnp.float32) ** block_scale(streams_of[3], (SECTIONS, TOKENS, TOP), ((0, 8), (1, 32)), -0.2, 0.2)), 0.05, 0.8),
        "bwd_ids": draw_bwd_ids(jax.random.fold_in(streams_of[11], 71), 0),
        "bwd_gates": jnp.clip(jnp.exp(math.log(0.8) - 2.7725887 * jax.random.uniform(streams_of[5], (SECTIONS, TOKENS, TOP), jnp.float32) ** block_scale(streams_of[5], (SECTIONS, TOKENS, TOP), ((0, 8), (1, 32)), -0.2, 0.2)), 0.05, 0.8),
        "gate_w": scatter_about(streams_of[6], (SECTIONS, D, EXPERTS * FF), D ** -0.5, 0.0625, ((0, 8), (2, 32))),
        "up_w": scatter_about(streams_of[7], (SECTIONS, D, EXPERTS * FF), D ** -0.5, 0.0625, ((0, 8), (2, 32))),
        "down_w": scatter_about(streams_of[8], (SECTIONS, EXPERTS * FF, D), FF ** -0.5, 0.125, ((0, 8), (1, 32))),
        "gate_pre": scatter_about(streams_of[9], (SECTIONS, SLOTS, EXPERTS * FF), 1.0, 6.0, ((0, 8), (2, 32))),
        "up_pre": scatter_about(streams_of[10], (SECTIONS, SLOTS, EXPERTS * FF), 1.0, 6.0, ((0, 8), (2, 32))),
    }


def slots_of(ids, expert):
    matches = ids == expert
    routed = jnp.any(matches, axis=1)
    blocks = routed.reshape(-1, TOK_DEV).astype(jnp.int32)
    position = (jnp.cumsum(blocks, axis=1) - 1).reshape(-1)
    block_ids = jnp.arange(TOKENS, dtype=jnp.int32) // TOK_DEV
    slot = jnp.where(routed, block_ids * CAP + position, SLOTS).astype(jnp.int32)
    return matches, slot


def place_rows(tokens, slot):
    empty = jnp.zeros((SLOTS, tokens.shape[1]), tokens.dtype)
    return empty.at[slot].set(tokens, mode="drop")


def take_rows(table, slot):
    return jnp.take(table, jnp.minimum(slot, SLOTS - 1).astype(jnp.int32), axis=0)


def rounded_sum(parts):
    rounded = lax.optimization_barrier(parts.astype(jnp.bfloat16))
    return jnp.sum(rounded.astype(jnp.float32), axis=0)


def section_layer(tokens, grads, ids_f, gates_f, ids_b, gates_b, w_gate, w_up, w_down, pre_gate, pre_up):
    mixed = jnp.zeros((TOKENS, D), jnp.float32)
    input_grad = jnp.zeros((TOKENS, D), jnp.float32)
    gate_grad = jnp.zeros((TOKENS, TOP), jnp.float32)
    for expert in range(EXPERTS):
        lo_col = expert * FF
        wg_e = w_gate[:, lo_col:lo_col + FF]
        wu_e = w_up[:, lo_col:lo_col + FF]
        wd_e = w_down[lo_col:lo_col + FF]
        matches, slot = slots_of(ids_f, expert)
        weights = jnp.sum(jnp.where(matches, gates_f, 0.0), axis=1)
        rows = place_rows(tokens, slot)
        gate_act = jnp.dot(rows, wg_e, preferred_element_type=jnp.float32)
        up_act = jnp.dot(rows, wu_e, preferred_element_type=jnp.float32)
        hidden = (jax.nn.silu(gate_act) * up_act).astype(jnp.bfloat16)
        parts = jnp.einsum("rsf,sfd->srd", hidden.reshape(SLOTS, SLICES, FF_DEV).astype(jnp.float32),
                           wd_e.reshape(SLICES, FF_DEV, D).astype(jnp.float32))
        expert_out = rounded_sum(parts)
        mixed = mixed + weights[:, None] * take_rows(expert_out, slot)

        matches_b, slot_b = slots_of(ids_b, expert)
        weights_b = jnp.sum(jnp.where(matches_b, gates_b, 0.0), axis=1)
        grad_rows = place_rows(grads, slot_b)
        saved_gate = pre_gate[:, lo_col:lo_col + FF].astype(jnp.float32)
        saved_up = pre_up[:, lo_col:lo_col + FF].astype(jnp.float32)
        grad_hidden = jnp.dot(grad_rows, wd_e.T, preferred_element_type=jnp.float32)
        sigmoid_gate = jax.nn.sigmoid(saved_gate)
        activated = saved_gate * sigmoid_gate
        dot_parts = jnp.sum((grad_hidden * activated * saved_up).reshape(SLOTS, SLICES, FF_DEV), axis=2)
        expert_dot = rounded_sum(dot_parts.T)
        grad_gate_act = (grad_hidden * saved_up * sigmoid_gate * (1.0 + saved_gate * (1.0 - sigmoid_gate))).astype(jnp.bfloat16)
        grad_up_act = (grad_hidden * activated).astype(jnp.bfloat16)
        grad_parts = jnp.einsum("rsf,dsf->srd", grad_gate_act.reshape(SLOTS, SLICES, FF_DEV).astype(jnp.float32),
                                wg_e.reshape(D, SLICES, FF_DEV).astype(jnp.float32))
        grad_parts = grad_parts + jnp.einsum("rsf,dsf->srd", grad_up_act.reshape(SLOTS, SLICES, FF_DEV).astype(jnp.float32),
                                             wu_e.reshape(D, SLICES, FF_DEV).astype(jnp.float32))
        expert_grad = rounded_sum(grad_parts)
        input_grad = input_grad + weights_b[:, None] * take_rows(expert_grad, slot_b)
        gate_grad = gate_grad + jnp.where(matches_b, take_rows(expert_dot, slot_b)[:, None], 0.0)
    return mixed.astype(jnp.bfloat16), input_grad.astype(jnp.bfloat16), gate_grad


def reference(act_in, cotangent, fwd_ids, fwd_gates, bwd_ids, bwd_gates, gate_w, up_w, down_w, gate_pre, up_pre):
    outputs = []
    grads = []
    gate_grads = []
    for section in range(SECTIONS):
        mixed, input_grad, gate_grad = section_layer(act_in[section], cotangent[section], fwd_ids[section], fwd_gates[section],
                                                   bwd_ids[section], bwd_gates[section], gate_w[section], up_w[section],
                                                   down_w[section], gate_pre[section], up_pre[section])
        outputs.append(mixed)
        grads.append(input_grad)
        gate_grads.append(gate_grad)
    next_act = jnp.roll(jnp.stack(outputs), 1, axis=0)
    prev_grad = jnp.roll(jnp.stack(grads), -1, axis=0)
    return next_act, prev_grad, jnp.stack(gate_grads)
```

```python
import jax
import jax.numpy as jnp
from jax import lax
from jax.experimental import pallas as pl
from jax.experimental.pallas import tpu as pltpu
from jax.sharding import PartitionSpec as P

MESH = pl.DeviceIdType.MESH
BF = jnp.bfloat16
F32 = jnp.float32

D = 7168
NC = 7
CH = D // NC
NJ = 2 * NC
TOK = 128
FFD = 128
SUB = 16
PW = 640
ROWS = 320

(Z, A_L, A_R, FA_L, FA_R, B_L, B_R, FB_L, FB_R) = range(9)
(BO_L, BO_R, BN_L, BN_R, AO_L, AO_R, AN_L, AN_R, FIN0, FIN1) = range(9, 19)
NK = 19
(DBO, DBN_L, DBN_R, DAO, DAN_L, DAN_R, DZ, WT0, WT1) = range(9)
NX = 9

RS_LAG = 12
STEPS = NJ + RS_LAG + 6


def iota(shape, dim):
    return lax.broadcasted_iota(jnp.int32, shape, dim)


def onehot(cond):
    return jnp.where(cond, 1.0, 0.0).astype(BF)


def nn(a, b):
    return jnp.dot(a, b, preferred_element_type=F32)


def nt(a, b):
    return lax.dot_general(a, b, (((1,), (1,)), ((), ())), preferred_element_type=F32)


def relay_kernel(
    act, cot, fids, fgates, bids, bgates, gw, uw, dw, gpre, upre,
    fin_out, wt_out, gg_out,
    tok, gu, wd, ids, gates, pre, pref, gbuf, zbuf, qbuf, bo, bn, ao, an, fbuf,
    lhs, pt, wts, perm_u, perm_p, xbuf, acc, accb, hid, ggu, dbuf, dbo, dbn, dao, dan, dfin, dz, ggb,
    ssem, rsem, xs, xr, lsem, osem,
):
    sec = lax.axis_index("section")
    exp = lax.axis_index("expert")
    core = lax.rem(sec, 2)
    zlo = exp // 16
    cx = lax.rem(exp // 4, 4)
    cy = lax.rem(exp, 4)
    a = cx * (1 - core) + cy * core
    b = cy * (1 - core) + cx * core
    al, ar, aopp = lax.rem(a + 3, 4), lax.rem(a + 1, 4), lax.rem(a + 2, 4)
    bl, br, bopp = lax.rem(b + 3, 4), lax.rem(b + 1, 4), lax.rem(b + 2, 4)

    def plane(ap, bp):
        return zlo * 16 + ap * (4 - 3 * core) + bp * (1 + 3 * core)

    partner = exp + 16 - 32 * zlo
    dev_al, dev_ar = {"expert": plane(al, b)}, {"expert": plane(ar, b)}
    dev_bl, dev_br = {"expert": plane(a, bl)}, {"expert": plane(a, br)}
    dev_z = {"expert": partner}
    nxt, prv = lax.rem(sec + 1, 8), lax.rem(sec + 7, 8)

    def load(src, dst, k):
        return pltpu.make_async_copy(src, dst, lsem.at[k])

    small = [
        load(fids.at[0], ids.at[0], NJ),
        load(bids.at[0], ids.at[1], NJ + 1),
        load(fgates.at[0], gates.at[0], NJ + 2),
        load(bgates.at[0], gates.at[1], NJ + 3),
    ]
    big = [
        load(gw.at[0], gu.at[:, pl.ds(0, FFD)], NJ + 4),
        load(uw.at[0], gu.at[:, pl.ds(FFD, FFD)], NJ + 5),
        load(dw.at[0], wd, NJ + 6),
        load(gpre.at[0], pre.at[:, pl.ds(0, FFD)], NJ + 7),
        load(upre.at[0], pre.at[:, pl.ds(FFD, FFD)], NJ + 8),
    ]
    toks = []
    for j in range(NJ):
        src = act if j < NC else cot
        toks.append(load(src.at[0, :, pl.ds((j % NC) * CH, CH)], tok.at[j], j))
    for c in small:
        c.start()
    for c in toks[:NC]:
        c.start()
    for c in big[:2]:
        c.start()
    for c in toks[NC:]:
        c.start()
    for c in big[2:]:
        c.start()

    barrier = pltpu.get_barrier_semaphore()
    peers = [dev_al, dev_ar, dev_bl, dev_br, dev_z]
    for s in (nxt, prv):
        peers.append({"section": s, "expert": exp})
        peers.append({"section": s, "expert": partner})
    for dev in peers:
        pl.semaphore_signal(barrier, inc=1, device_id=dev, device_id_type=MESH)

    for c in small:
        c.wait()
    lower = onehot(iota((TOK, TOK), 0) >= iota((TOK, TOK), 1))
    lane = iota((TOK, TOK), 1)
    q0 = iota((160, TOK), 0)
    spread = onehot(
        iota((160, TOK), 1) == (q0 >> 3) + jnp.where(q0 >= 80, 6, 0)
    )
    for p in range(2):
        table = jnp.zeros((TOK, TOK), F32)
        weighted = jnp.zeros((TOK, TOK), F32)
        for h in range(2):
            e = zlo if h == 0 else 1 - zlo
            match = ids[p] == e
            routed = jnp.max(jnp.where(match, 1.0, 0.0), axis=1, keepdims=True)
            w = jnp.sum(jnp.where(match, gates[p], 0.0), axis=1, keepdims=True)
            wide = jnp.broadcast_to(routed, (TOK, TOK))
            rank = nn(lower, wide.astype(BF)).astype(jnp.int32) - 1 + 16 * h
            placed = jnp.where((lane == rank) & (wide > 0.5), 1.0, 0.0)
            table = table + placed
            weighted = weighted + placed * w
        pt[p] = table.astype(BF)
        wts[p] = weighted
        lhs[p] = nt(spread, table.astype(BF)).astype(BF)
    pl.semaphore_wait(barrier, len(peers))

    def extra(src, dst, k, dev):
        return pltpu.make_async_remote_copy(
            src_ref=src, dst_ref=dst, send_sem=xs.at[k], recv_sem=xr.at[k],
            device_id=dev, device_id_type=MESH,
        )

    wt_copies = [
        extra(wts.at[0], wt_out.at[0], WT0, {"section": nxt, "expert": exp}),
        extra(wts.at[1], wt_out.at[1], WT1, {"section": prv, "expert": exp}),
    ]
    for c in wt_copies:
        c.start()

    def ring(src, dst, k, j, dev):
        return pltpu.make_async_remote_copy(
            src_ref=src, dst_ref=dst, send_sem=ssem.at[k, j], recv_sem=rsem.at[k, j],
            device_id=dev, device_id_type=MESH,
        )

    def out(k, j):
        if k == Z:
            return ring(zbuf.at[j], gbuf.at[j, b, a, 1], k, j, dev_z)
        if k == A_L:
            return ring(gbuf.at[j, b, a], gbuf.at[j, b, a], k, j, dev_ar)
        if k == A_R:
            return ring(gbuf.at[j, b, a], gbuf.at[j, b, a], k, j, dev_al)
        if k == FA_L:
            return ring(gbuf.at[j, b, al, 0], gbuf.at[j, b, al, 0], k, j, dev_ar)
        if k == FA_R:
            return ring(gbuf.at[j, b, ar, 1], gbuf.at[j, b, ar, 1], k, j, dev_al)
        if k == B_L:
            return ring(gbuf.at[j, b], gbuf.at[j, b], k, j, dev_br)
        if k == B_R:
            return ring(gbuf.at[j, b], gbuf.at[j, b], k, j, dev_bl)
        if k == FB_L:
            half = gbuf.at[j, bl, pl.ds(0, 2)]
            return ring(half, half, k, j, dev_br)
        if k == FB_R:
            half = gbuf.at[j, br, pl.ds(2, 2)]
            return ring(half, half, k, j, dev_bl)
        if k == BO_L:
            return ring(qbuf.at[j, bopp, pl.ds(0, 2)], bo.at[j, 0], k, j, dev_br)
        if k == BO_R:
            return ring(qbuf.at[j, bopp, pl.ds(2, 2)], bo.at[j, 1], k, j, dev_bl)
        if k == BN_L:
            return ring(qbuf.at[j, br], bn.at[j, 0], k, j, dev_br)
        if k == BN_R:
            return ring(qbuf.at[j, bl], bn.at[j, 1], k, j, dev_bl)
        if k == AO_L:
            return ring(qbuf.at[j, b, aopp, 0], ao.at[j, 0], k, j, dev_ar)
        if k == AO_R:
            return ring(qbuf.at[j, b, aopp, 1], ao.at[j, 1], k, j, dev_al)
        if k == AN_L:
            return ring(qbuf.at[j, b, ar], an.at[j, 0], k, j, dev_ar)
        if k == AN_R:
            return ring(qbuf.at[j, b, al], an.at[j, 1], k, j, dev_al)
        to = jnp.where(j < NC, nxt, prv)
        h = k - FIN0
        dev = {"section": to, "expert": exp if h == 0 else partner}
        return ring(fbuf.at[j, h], fin_out.at[j, h], k, j, dev)

    def arrived(k, j):
        dst = {
            Z: lambda: gbuf.at[j, b, a, 1],
            A_L: lambda: gbuf.at[j, b, al],
            A_R: lambda: gbuf.at[j, b, ar],
            FA_L: lambda: gbuf.at[j, b, aopp, 0],
            FA_R: lambda: gbuf.at[j, b, aopp, 1],
            B_L: lambda: gbuf.at[j, bl],
            B_R: lambda: gbuf.at[j, br],
            FB_L: lambda: gbuf.at[j, bopp, pl.ds(0, 2)],
            FB_R: lambda: gbuf.at[j, bopp, pl.ds(2, 2)],
            BO_L: lambda: bo.at[j, 0],
            BO_R: lambda: bo.at[j, 1],
            BN_L: lambda: bn.at[j, 0],
            BN_R: lambda: bn.at[j, 1],
            AO_L: lambda: ao.at[j, 0],
            AO_R: lambda: ao.at[j, 1],
            AN_L: lambda: an.at[j, 0],
            AN_R: lambda: an.at[j, 1],
            FIN0: lambda: fin_out.at[j, 0],
            FIN1: lambda: fin_out.at[j, 1],
        }[k]()
        ring(dst, dst, k, j, dev_z).wait_recv()

    def send(*kinds, j):
        for k in kinds:
            out(k, j).start()

    def sent(*kinds, j):
        for k in kinds:
            out(k, j).wait_send()

    row_k = iota((SUB, FFD), 0) & 7

    def pack(j):
        p = j // NC
        load(act.at[0, :, pl.ds(0, CH)], tok.at[j], j).wait()
        y = nn(lhs[p], tok[j])
        for h in range(2):
            for c in range(5):
                r = (h * 5 + c) * SUB
                v = y[r:r + SUB, 0:FFD]
                for k in range(1, 8):
                    v = jnp.where(row_k == k, y[r:r + SUB, k * FFD:(k + 1) * FFD], v)
                if h == 0:
                    gbuf[j, b, a, 0, :, c * FFD:(c + 1) * FFD] = v.astype(BF)
                else:
                    zbuf[j, :, c * FFD:(c + 1) * FFD] = v.astype(BF)

    def tables():
        o = iota((256, 256), 0)
        i = iota((256, 256), 1)
        perm_u[...] = onehot(i == ((o & 31) >> 1) * 16 + (o & 1) * 8 + (o >> 5))
        perm_p[...] = onehot(o == ((i & 31) >> 1) * 16 + (i & 1) * 8 + (i >> 5))

    def saved():
        for c in big[3:]:
            c.wait()
        i = iota((ROWS, ROWS), 0)
        hc = i >> 5
        h = jnp.where(hc >= 5, 1, 0)
        c5 = hc - 5 * h
        bp = (i >> 3) & 3
        ap = (i >> 1) & 3
        xy = ap * (4 - 3 * core) + bp * (1 + 3 * core)
        pln = zlo + h - 2 * zlo * h
        src = (pln * 16 + xy) * 10 + c5 * 2 + (i & 1)
        pref[...] = nn(onehot(iota((ROWS, ROWS), 1) == src), pre[...])

    def unpack(j):
        for h in range(2):
            g = gbuf[j, :, :, h].reshape(256, PW)
            r = nn(perm_u[...], g).astype(BF)
            for c in range(5):
                for k in range(8):
                    xbuf[(h * 5 + c) * 32:(h * 5 + c) * 32 + 32, k * FFD:(k + 1) * FFD] = (
                        r[k * 32:(k + 1) * 32, c * FFD:(c + 1) * FFD]
                    )

    def repack(j, o):
        o = o.astype(BF)
        for h in range(2):
            cols = []
            for c in range(5):
                r0 = (h * 5 + c) * 32
                cols.append(
                    jnp.concatenate(
                        [o[r0:r0 + 32, k * FFD:(k + 1) * FFD] for k in range(8)], axis=0
                    )
                )
            r = jnp.concatenate(cols, axis=1)
            q = nn(perm_p[...], r).astype(BF)
            qbuf[j, :, :, h] = q.reshape(4, 4, SUB, PW)

    def forward_rows(j):
        i = pl.multiple_of(j * CH, CH)

        @pl.when(j == 0)
        def _():
            for c in big[:2]:
                c.wait()
            acc[...] = nn(xbuf[...], gu[pl.ds(i, CH), :])

        @pl.when(j > 0)
        def _():
            acc[...] += nn(xbuf[...], gu[pl.ds(i, CH), :])

        @pl.when(j == NC - 1)
        def _():
            big[2].wait()
            g = acc[:, 0:FFD]
            hid[...] = (g / (1.0 + jnp.exp(-g)) * acc[:, FFD:2 * FFD]).astype(BF)

    def backward_rows(j):
        i = pl.multiple_of((j - NC) * CH, CH)

        @pl.when(j == NC)
        def _():
            accb[...] = nt(xbuf[...], wd[:, pl.ds(i, CH)])

        @pl.when(j > NC)
        def _():
            accb[...] += nt(xbuf[...], wd[:, pl.ds(i, CH)])

        @pl.when(j == NJ - 1)
        def _():
            gh = accb[...]
            g = pref[:, 0:FFD]
            u = pref[:, FFD:2 * FFD]
            s = 1.0 / (1.0 + jnp.exp(-g))
            silu = g * s
            ggu[:, 0:FFD] = (gh * u * s * (1.0 + g * (1.0 - s))).astype(BF)
            ggu[:, FFD:2 * FFD] = (gh * silu).astype(BF)
            dots = jnp.sum(gh * silu * u, axis=1, keepdims=True)
            at = iota((ROWS, FFD), 1) == (iota((ROWS, FFD), 0) >> 5)
            spot = jnp.where(at, jnp.broadcast_to(dots, (ROWS, FFD)), 0.0).astype(BF)
            o = iota((FFD, ROWS), 0)
            i2 = iota((FFD, ROWS), 1) & 31
            pick = onehot(((o & 7) < 2) & (i2 == (o >> 3) * 2 + (o & 7)))
            dbuf[...] = nn(pick, spot).reshape(4, 4, 8, FFD)

    def f32(v):
        return v.astype(F32)

    @pl.loop(0, STEPS)
    def _(t):
        def event(lag, lo=0, hi=NJ):
            def wrap(f):
                @pl.when((t - lag >= lo) & (t - lag < hi))
                def _():
                    f(t - lag)
            return wrap

        @event(0)
        def _(j):
            pack(j)
            send(Z, j=j)

            @pl.when(j == 1)
            def _():
                tables()

        @event(1)
        def _(j):
            arrived(Z, j)
            send(A_L, A_R, j=j)

        @event(2)
        def _(j):
            arrived(A_L, j)
            send(FA_L, j=j)
            arrived(A_R, j)
            send(FA_R, j=j)

        @event(3)
        def _(j):
            arrived(FA_L, j)
            arrived(FA_R, j)
            send(B_L, B_R, j=j)

        @event(4)
        def _(j):
            arrived(B_L, j)
            send(FB_L, j=j)
            arrived(B_R, j)
            send(FB_R, j=j)

        @event(RS_LAG)
        def _(j):
            @pl.when(j < NC)
            def _():
                i = pl.multiple_of(j * CH, CH)
                repack(j, nn(hid[...], wd[:, pl.ds(i, CH)]))

            @pl.when(j >= NC)
            def _():
                i = pl.multiple_of((j - NC) * CH, CH)
                repack(j, nt(ggu[...], gu[pl.ds(i, CH), :]))

            send(BO_L, BO_R, j=j)

            @pl.when(j == NC)
            def _():
                extra(dbuf.at[bopp], dbo, DBO, dev_br).start()

        @event(RS_LAG + 1)
        def _(j):
            arrived(BO_L, j)
            qbuf[j, br, 0:2] = (f32(qbuf[j, br, 0:2]) + f32(bo[j, 0])).astype(BF)
            send(BN_L, j=j)
            arrived(BO_R, j)
            qbuf[j, bl, 2:4] = (f32(qbuf[j, bl, 2:4]) + f32(bo[j, 1])).astype(BF)
            send(BN_R, j=j)

            @pl.when(j == NC)
            def _():
                extra(dbuf.at[bopp], dbo, DBO, dev_br).wait()
                dbuf[br] = dbuf[br] + dbo[...]
                extra(dbuf.at[br], dbn.at[0], DBN_L, dev_br).start()
                extra(dbuf.at[bl], dbn.at[1], DBN_R, dev_bl).start()

        @event(RS_LAG + 2)
        def _(j):
            arrived(BN_L, j)
            arrived(BN_R, j)
            qbuf[j, b] = (f32(qbuf[j, b]) + f32(bn[j, 0]) + f32(bn[j, 1])).astype(BF)
            send(AO_L, AO_R, j=j)

            @pl.when(j == NC)
            def _():
                extra(dbuf.at[br], dbn.at[0], DBN_L, dev_br).wait()
                extra(dbuf.at[bl], dbn.at[1], DBN_R, dev_bl).wait()
                dbuf[b] = dbuf[b] + dbn[0] + dbn[1]
                extra(dbuf.at[b, aopp], dao, DAO, dev_ar).start()

        @event(RS_LAG + 3)
        def _(j):
            arrived(AO_L, j)
            qbuf[j, b, ar, 0] = (f32(qbuf[j, b, ar, 0]) + f32(ao[j, 0])).astype(BF)
            send(AN_L, j=j)
            arrived(AO_R, j)
            qbuf[j, b, al, 1] = (f32(qbuf[j, b, al, 1]) + f32(ao[j, 1])).astype(BF)
            send(AN_R, j=j)

            @pl.when(j == NC)
            def _():
                extra(dbuf.at[b, aopp], dao, DAO, dev_ar).wait()
                dbuf[b, ar] = dbuf[b, ar] + dao[...]
                extra(dbuf.at[b, ar], dan.at[0], DAN_L, dev_ar).start()
                extra(dbuf.at[b, al], dan.at[1], DAN_R, dev_al).start()

        @event(RS_LAG + 4)
        def _(j):
            arrived(AN_L, j)
            arrived(AN_R, j)
            fbuf[j] = (f32(qbuf[j, b, a]) + f32(an[j, 0]) + f32(an[j, 1])).astype(BF)
            send(FIN0, FIN1, j=j)

            @pl.when(j == NC)
            def _():
                extra(dbuf.at[b, ar], dan.at[0], DAN_L, dev_ar).wait()
                extra(dbuf.at[b, al], dan.at[1], DAN_R, dev_al).wait()
                dfin[...] = dbuf[b, a] + dan[0] + dan[1]
                extra(dfin, dz, DZ, dev_z).start()

        @event(RS_LAG + 5)
        def _(j):
            arrived(FIN0, j)
            arrived(FIN1, j)
            sent(BO_L, BO_R, BN_L, BN_R, AO_L, AO_R, AN_L, AN_R, FIN0, FIN1, j=j)

            @pl.when(j == NC)
            def _():
                extra(dfin, dz, DZ, dev_z).wait()
                la = iota((8, FFD), 1)
                mine = jnp.where(la < 5, dfin[...], dz[...])
                i = iota((TOK, TOK), 0)
                l = iota((TOK, TOK), 1)
                total = jnp.zeros((TOK, TOK), F32)
                for par in range(2):
                    h = i >> 4
                    ok = (i < 32) & ((i & 1) == par) & ((i & 15) < 10)
                    to = onehot(ok & (l == h * 5 + ((i & 15) >> 1)))
                    total = total + nn(pt[1], to) * mine[par:par + 1, :]
                d0 = jnp.sum(jnp.where(l < 5, total, 0.0), axis=1, keepdims=True)
                d1 = jnp.sum(jnp.where(l >= 5, total, 0.0), axis=1, keepdims=True)
                which = ids[1]
                ggb[...] = jnp.where(which == zlo, d0, 0.0) + jnp.where(
                    which == 1 - zlo, d1, 0.0
                )
                pltpu.make_async_copy(ggb, gg_out, osem).start()

        @event(5)
        def _(j):
            @pl.when(j == 0)
            def _():
                saved()

            arrived(FB_L, j)
            arrived(FB_R, j)
            unpack(j)

            @pl.when(j < NC)
            def _():
                forward_rows(j)

            @pl.when(j >= NC)
            def _():
                backward_rows(j)

            sent(Z, A_L, A_R, FA_L, FA_R, B_L, B_R, FB_L, FB_R, j=j)

    for c in wt_copies:
        c.wait()
    pltpu.make_async_copy(ggb, gg_out, osem).wait()


def relay(*args):
    any_spec = pl.BlockSpec(memory_space=pl.ANY)
    vmem = pltpu.VMEM
    return pl.pallas_call(
        relay_kernel,
        out_shape=(
            jax.ShapeDtypeStruct((NJ, 2, SUB, PW), BF),
            jax.ShapeDtypeStruct((2, TOK, TOK), F32),
            jax.ShapeDtypeStruct((TOK, 8), F32),
        ),
        in_specs=[any_spec] * 11,
        out_specs=(any_spec,) * 3,
        scratch_shapes=[
            vmem((NJ, TOK, CH), BF),
            vmem((D, 2 * FFD), BF),
            vmem((FFD, D), BF),
            vmem((2, TOK, 8), jnp.int32),
            vmem((2, TOK, 8), F32),
            vmem((ROWS, 2 * FFD), BF),
            vmem((ROWS, 2 * FFD), F32),
            vmem((NJ, 4, 4, 2, SUB, PW), BF),
            vmem((NJ, SUB, PW), BF),
            vmem((NJ, 4, 4, 2, SUB, PW), BF),
            vmem((NJ, 2, 2, 2, SUB, PW), BF),
            vmem((NJ, 2, 4, 2, SUB, PW), BF),
            vmem((NJ, 2, SUB, PW), BF),
            vmem((NJ, 2, 2, SUB, PW), BF),
            vmem((NJ, 2, SUB, PW), BF),
            vmem((2, 160, TOK), BF),
            vmem((2, TOK, TOK), BF),
            vmem((2, TOK, TOK), F32),
            vmem((256, 256), BF),
            vmem((256, 256), BF),
            vmem((ROWS, CH), BF),
            vmem((ROWS, 2 * FFD), F32),
            vmem((ROWS, FFD), F32),
            vmem((ROWS, FFD), BF),
            vmem((ROWS, 2 * FFD), BF),
            vmem((4, 4, 8, FFD), F32),
            vmem((4, 8, FFD), F32),
            vmem((2, 4, 8, FFD), F32),
            vmem((8, FFD), F32),
            vmem((2, 8, FFD), F32),
            vmem((8, FFD), F32),
            vmem((8, FFD), F32),
            vmem((TOK, 8), F32),
            pltpu.SemaphoreType.DMA((NK, NJ)),
            pltpu.SemaphoreType.DMA((NK, NJ)),
            pltpu.SemaphoreType.DMA((NX,)),
            pltpu.SemaphoreType.DMA((NX,)),
            pltpu.SemaphoreType.DMA((NJ + 9,)),
            pltpu.SemaphoreType.DMA,
        ],
        compiler_params=pltpu.CompilerParams(
            collective_id=0, has_side_effects=True, vmem_limit_bytes=62 * 2**20
        ),
        name="relay",
    )(*args)


def spread_kernel(ff, fb, wt, gg, next_ref, prev_ref, gg_ref, sel, lhs):
    @pl.when(pl.program_id(0) == 0)
    def _():
        gg_ref[0] = gg[...]
        o = iota((256, 160), 0)
        v = iota((256, 160), 1)
        slot = (v >> 3) + jnp.where(v >= 80, 6, 0)
        sel[...] = onehot(((v & 7) == (o >> 5)) & ((o & 31) == slot))
        for p in range(2):
            w = wt[p][:, 0:32]
            hi = w.astype(BF)
            lhs[p, :, 0:32] = hi
            lhs[p, :, 32:64] = (w - hi.astype(F32)).astype(BF)

    for p, (src, dst) in enumerate(((ff, next_ref), (fb, prev_ref))):
        v = jnp.concatenate(
            [src[0, h, :, c * FFD:(c + 1) * FFD] for h in range(2) for c in range(5)], axis=0
        )
        u = nn(sel[...], v).astype(BF)
        row = jnp.concatenate([u[k * 32:(k + 1) * 32] for k in range(8)], axis=1)
        both = jnp.concatenate([row, row], axis=0)
        dst[0] = nn(lhs[p], both).astype(BF)


def dense(fin, wt, gg):
    return pl.pallas_call(
        spread_kernel,
        grid=(NC,),
        out_shape=(
            jax.ShapeDtypeStruct((1, TOK, D), BF),
            jax.ShapeDtypeStruct((1, TOK, D), BF),
            jax.ShapeDtypeStruct((1, TOK, 8), F32),
        ),
        in_specs=[
            pl.BlockSpec((1, 2, SUB, PW), lambda i: (i, 0, 0, 0)),
            pl.BlockSpec((1, 2, SUB, PW), lambda i: (i + NC, 0, 0, 0)),
            pl.BlockSpec((2, TOK, TOK), lambda i: (0, 0, 0)),
            pl.BlockSpec((TOK, 8), lambda i: (0, 0)),
        ],
        out_specs=(
            pl.BlockSpec((1, TOK, CH), lambda i: (0, 0, i)),
            pl.BlockSpec((1, TOK, CH), lambda i: (0, 0, i)),
            pl.BlockSpec((1, TOK, 8), lambda i: (0, 0, 0)),
        ),
        scratch_shapes=[pltpu.VMEM((256, 160), BF), pltpu.VMEM((2, TOK, 64), BF)],
        name="dense",
    )(fin, fin, wt, gg)


def body(*args):
    fin, wt, gg = relay(*args)
    return dense(fin, wt, gg)


def solution(mesh):
    rows = P("section", "expert", None)
    cols = P("section", None, "expert")
    return jax.shard_map(
        body,
        mesh=mesh,
        in_specs=(rows,) * 6 + (cols, cols, rows, cols, cols),
        out_specs=(rows,) * 3,
        check_vma=False,
    )
```

```python
import jax
import jax.numpy as jnp
from jax import lax
from jax.experimental import pallas as pl
from jax.experimental.pallas import tpu as pltpu
from jax.sharding import PartitionSpec as P

MESH = pl.DeviceIdType.MESH
BF = jnp.bfloat16
F32 = jnp.float32

D = 7168
NC = 7
CH = D // NC
NJ = 2 * NC
TOK = 128
FFD = 128
SUB = 16
PW = 640
ROWS = 320

(Z, A_L, A_R, FA_L, FA_R, B_L, B_R, FB_L, FB_R) = range(9)
(BO_L, BO_R, BN_L, BN_R, AO_L, AO_R, AN_L, AN_R, FIN0, FIN1) = range(9, 19)
NK = 19
(DBO, DBN_L, DBN_R, DAO, DAN_L, DAN_R, DZ, WT0, WT1) = range(9)
NX = 9

E1, E2, E3, E4, E5 = 1, 3, 5, 7, 9
R0 = E5 + NC
R1, R2, R3, R4, R5 = R0 + 2, R0 + 4, R0 + 6, R0 + 8, R0 + 10
STEPS = NJ + R5


def iota(shape, dim):
    return lax.broadcasted_iota(jnp.int32, shape, dim)


def onehot(cond):
    return jnp.where(cond, 1.0, 0.0).astype(BF)


def nn(a, b):
    return jnp.dot(a, b, preferred_element_type=F32)


def nt(a, b):
    return lax.dot_general(a, b, (((1,), (1,)), ((), ())), preferred_element_type=F32)


def relay_kernel(
    act, cot, fids, fgates, bids, bgates, gw, uw, dw, gpre, upre,
    u_out, wt_out, gg_out,
    tok, gu, wd, ids, gates, pre, pref, gbuf, zbuf, qbuf, bo, bn, ao, an, fbuf, fin, ubuf, sel,
    lhs, rk, wts, perm_u, perm_p, xbuf, acc, accb, hid, ggu, dbuf, dbo, dbn, dao, dan, dfin, dz, ggb,
    ssem, rsem, xs, xr, lsem, osem, usem,
):
    sec = lax.axis_index("section")
    exp = lax.axis_index("expert")
    core = lax.rem(sec, 2)
    zlo = exp // 16
    cx = lax.rem(exp // 4, 4)
    cy = lax.rem(exp, 4)
    a = cx * (1 - core) + cy * core
    b = cy * (1 - core) + cx * core
    al, ar, aopp = lax.rem(a + 3, 4), lax.rem(a + 1, 4), lax.rem(a + 2, 4)
    bl, br, bopp = lax.rem(b + 3, 4), lax.rem(b + 1, 4), lax.rem(b + 2, 4)

    def plane(ap, bp):
        return zlo * 16 + ap * (4 - 3 * core) + bp * (1 + 3 * core)

    partner = exp + 16 - 32 * zlo
    dev_al, dev_ar = {"expert": plane(al, b)}, {"expert": plane(ar, b)}
    dev_bl, dev_br = {"expert": plane(a, bl)}, {"expert": plane(a, br)}
    dev_z = {"expert": partner}
    nxt, prv = lax.rem(sec + 1, 8), lax.rem(sec + 7, 8)

    def load(src, dst, k):
        return pltpu.make_async_copy(src, dst, lsem.at[k])

    small = [
        load(fids.at[0], ids.at[0], NJ),
        load(bids.at[0], ids.at[1], NJ + 1),
        load(fgates.at[0], gates.at[0], NJ + 2),
        load(bgates.at[0], gates.at[1], NJ + 3),
    ]
    big = [
        load(gw.at[0], gu.at[:, pl.ds(0, FFD)], NJ + 4),
        load(uw.at[0], gu.at[:, pl.ds(FFD, FFD)], NJ + 5),
        load(dw.at[0], wd, NJ + 6),
        load(gpre.at[0], pre.at[:, pl.ds(0, FFD)], NJ + 7),
        load(upre.at[0], pre.at[:, pl.ds(FFD, FFD)], NJ + 8),
    ]
    toks = []
    for j in range(NJ):
        src = act if j < NC else cot
        toks.append(load(src.at[0, :, pl.ds((j % NC) * CH, CH)], tok.at[j], j))
    for c in small:
        c.start()
    for c in toks[:NC]:
        c.start()
    for c in big[:2]:
        c.start()
    for c in toks[NC:]:
        c.start()
    for c in big[2:]:
        c.start()

    barrier = pltpu.get_barrier_semaphore()
    peers = [dev_al, dev_ar, dev_bl, dev_br, dev_z]
    for s in (nxt, prv):
        peers.append({"section": s, "expert": exp})
        peers.append({"section": s, "expert": partner})
    for dev in peers:
        pl.semaphore_signal(barrier, inc=1, device_id=dev, device_id_type=MESH)

    for c in small:
        c.wait()
    upper = onehot(iota((TOK, TOK), 0) <= iota((TOK, TOK), 1))
    slot16 = iota((16, TOK), 0)
    row160 = iota((160, TOK), 0)
    for p in range(2):
        ranks = []
        for h in range(2):
            e = zlo if h == 0 else 1 - zlo
            match = ids[p] == e
            routed = jnp.max(jnp.where(match, 1.0, 0.0), axis=0, keepdims=True)
            w = jnp.sum(jnp.where(match, gates[p], 0.0), axis=0, keepdims=True)
            count = nn(jnp.broadcast_to(routed, (8, TOK)).astype(BF), upper)
            rank = jnp.where(routed > 0.5, count.astype(jnp.int32) - 1, -1)
            rk[p, h] = rank
            wts[p, h * 16:h * 16 + 16] = jnp.where(slot16 == rank[0:1], w, 0.0)
            ranks.append(rank[0:1])
        low = (row160 >> 3) == ranks[0]
        high = ((row160 >> 3) - 10) == ranks[1]
        lhs[p] = jnp.where(row160 < 80, jnp.where(low, 1.0, 0.0), jnp.where(high, 1.0, 0.0)).astype(BF)
    pl.semaphore_wait(barrier, len(peers))

    def extra(src, dst, k, dev):
        return pltpu.make_async_remote_copy(
            src_ref=src, dst_ref=dst, send_sem=xs.at[k], recv_sem=xr.at[k],
            device_id=dev, device_id_type=MESH,
        )

    wt_copies = [
        extra(wts.at[0], wt_out.at[0], WT0, {"section": nxt, "expert": exp}),
        extra(wts.at[1], wt_out.at[1], WT1, {"section": prv, "expert": exp}),
    ]
    for c in wt_copies:
        c.start()

    def ring(src, dst, k, j, dev):
        return pltpu.make_async_remote_copy(
            src_ref=src, dst_ref=dst, send_sem=ssem.at[k, j], recv_sem=rsem.at[k, j],
            device_id=dev, device_id_type=MESH,
        )

    def out(k, j):
        if k == Z:
            return ring(zbuf.at[j], gbuf.at[j, b, a, 1], k, j, dev_z)
        if k == A_L:
            return ring(gbuf.at[j, b, a], gbuf.at[j, b, a], k, j, dev_ar)
        if k == A_R:
            return ring(gbuf.at[j, b, a], gbuf.at[j, b, a], k, j, dev_al)
        if k == FA_L:
            return ring(gbuf.at[j, b, al, 0], gbuf.at[j, b, al, 0], k, j, dev_ar)
        if k == FA_R:
            return ring(gbuf.at[j, b, ar, 1], gbuf.at[j, b, ar, 1], k, j, dev_al)
        if k == B_L:
            return ring(gbuf.at[j, b], gbuf.at[j, b], k, j, dev_br)
        if k == B_R:
            return ring(gbuf.at[j, b], gbuf.at[j, b], k, j, dev_bl)
        if k == FB_L:
            half = gbuf.at[j, bl, pl.ds(0, 2)]
            return ring(half, half, k, j, dev_br)
        if k == FB_R:
            half = gbuf.at[j, br, pl.ds(2, 2)]
            return ring(half, half, k, j, dev_bl)
        if k == BO_L:
            return ring(qbuf.at[j, bopp, pl.ds(0, 2)], bo.at[j, 0], k, j, dev_br)
        if k == BO_R:
            return ring(qbuf.at[j, bopp, pl.ds(2, 2)], bo.at[j, 1], k, j, dev_bl)
        if k == BN_L:
            return ring(qbuf.at[j, br], bn.at[j, 0], k, j, dev_br)
        if k == BN_R:
            return ring(qbuf.at[j, bl], bn.at[j, 1], k, j, dev_bl)
        if k == AO_L:
            return ring(qbuf.at[j, b, aopp, 0], ao.at[j, 0], k, j, dev_ar)
        if k == AO_R:
            return ring(qbuf.at[j, b, aopp, 1], ao.at[j, 1], k, j, dev_al)
        if k == AN_L:
            return ring(qbuf.at[j, b, ar], an.at[j, 0], k, j, dev_ar)
        if k == AN_R:
            return ring(qbuf.at[j, b, al], an.at[j, 1], k, j, dev_al)
        to = jnp.where(j < NC, nxt, prv)
        h = k - FIN0
        dev = {"section": to, "expert": exp if h == 0 else partner}
        return ring(fbuf.at[j, h], fin.at[j, h], k, j, dev)

    def arrived(k, j):
        dst = {
            Z: lambda: gbuf.at[j, b, a, 1],
            A_L: lambda: gbuf.at[j, b, al],
            A_R: lambda: gbuf.at[j, b, ar],
            FA_L: lambda: gbuf.at[j, b, aopp, 0],
            FA_R: lambda: gbuf.at[j, b, aopp, 1],
            B_L: lambda: gbuf.at[j, bl],
            B_R: lambda: gbuf.at[j, br],
            FB_L: lambda: gbuf.at[j, bopp, pl.ds(0, 2)],
            FB_R: lambda: gbuf.at[j, bopp, pl.ds(2, 2)],
            BO_L: lambda: bo.at[j, 0],
            BO_R: lambda: bo.at[j, 1],
            BN_L: lambda: bn.at[j, 0],
            BN_R: lambda: bn.at[j, 1],
            AO_L: lambda: ao.at[j, 0],
            AO_R: lambda: ao.at[j, 1],
            AN_L: lambda: an.at[j, 0],
            AN_R: lambda: an.at[j, 1],
            FIN0: lambda: fin.at[j, 0],
            FIN1: lambda: fin.at[j, 1],
        }[k]()
        ring(dst, dst, k, j, dev_z).wait_recv()

    def send(*kinds, j):
        for k in kinds:
            out(k, j).start()

    def sent(*kinds, j):
        for k in kinds:
            out(k, j).wait_send()

    row_k = iota((SUB, FFD), 0) & 7

    def pack(j):
        p = j // NC
        load(act.at[0, :, pl.ds(0, CH)], tok.at[j], j).wait()
        y = nn(lhs[p], tok[j])
        for h in range(2):
            for c in range(5):
                r = (h * 5 + c) * SUB
                v = y[r:r + SUB, 0:FFD]
                for k in range(1, 8):
                    v = jnp.where(row_k == k, y[r:r + SUB, k * FFD:(k + 1) * FFD], v)
                if h == 0:
                    gbuf[j, b, a, 0, :, c * FFD:(c + 1) * FFD] = v.astype(BF)
                else:
                    zbuf[j, :, c * FFD:(c + 1) * FFD] = v.astype(BF)

    def tables():
        o = iota((256, 256), 0)
        i = iota((256, 256), 1)
        perm_u[...] = onehot(i == ((o & 31) >> 1) * 16 + (o & 1) * 8 + (o >> 5))
        perm_p[...] = onehot(o == ((i & 31) >> 1) * 16 + (i & 1) * 8 + (i >> 5))
        o = iota((256, 160), 0)
        v = iota((256, 160), 1)
        slot = (v >> 3) + jnp.where(v >= 80, 6, 0)
        sel[...] = onehot(((v & 7) == (o >> 5)) & ((o & 31) == slot))

    def saved():
        for c in big[3:]:
            c.wait()
        i = iota((ROWS, ROWS), 0)
        hc = i >> 5
        h = jnp.where(hc >= 5, 1, 0)
        c5 = hc - 5 * h
        bp = (i >> 3) & 3
        ap = (i >> 1) & 3
        xy = ap * (4 - 3 * core) + bp * (1 + 3 * core)
        pln = zlo + h - 2 * zlo * h
        src = (pln * 16 + xy) * 10 + c5 * 2 + (i & 1)
        pref[...] = nn(onehot(iota((ROWS, ROWS), 1) == src), pre[...])

    def unpack(j):
        for h in range(2):
            g = gbuf[j, :, :, h].reshape(256, PW)
            r = nn(perm_u[...], g).astype(BF)
            for c in range(5):
                for k in range(8):
                    xbuf[(h * 5 + c) * 32:(h * 5 + c) * 32 + 32, k * FFD:(k + 1) * FFD] = (
                        r[k * 32:(k + 1) * 32, c * FFD:(c + 1) * FFD]
                    )

    def repack(j, o):
        o = o.astype(BF)
        for h in range(2):
            cols = []
            for c in range(5):
                r0 = (h * 5 + c) * 32
                cols.append(
                    jnp.concatenate(
                        [o[r0:r0 + 32, k * FFD:(k + 1) * FFD] for k in range(8)], axis=0
                    )
                )
            r = jnp.concatenate(cols, axis=1)
            q = nn(perm_p[...], r).astype(BF)
            qbuf[j, :, :, h] = q.reshape(4, 4, SUB, PW)

    def forward_rows(j):
        i = pl.multiple_of(j * CH, CH)

        @pl.when(j == 0)
        def _():
            for c in big[:2]:
                c.wait()
            acc[...] = nn(xbuf[...], gu[pl.ds(i, CH), :])

        @pl.when(j > 0)
        def _():
            acc[...] += nn(xbuf[...], gu[pl.ds(i, CH), :])

        @pl.when(j == NC - 1)
        def _():
            big[2].wait()
            g = acc[:, 0:FFD]
            hid[...] = (g / (1.0 + jnp.exp(-g)) * acc[:, FFD:2 * FFD]).astype(BF)

    def backward_rows(j):
        i = pl.multiple_of((j - NC) * CH, CH)

        @pl.when(j == NC)
        def _():
            accb[...] = nt(xbuf[...], wd[:, pl.ds(i, CH)])

        @pl.when(j > NC)
        def _():
            accb[...] += nt(xbuf[...], wd[:, pl.ds(i, CH)])

        @pl.when(j == NJ - 1)
        def _():
            gh = accb[...]
            g = pref[:, 0:FFD]
            u = pref[:, FFD:2 * FFD]
            s = 1.0 / (1.0 + jnp.exp(-g))
            silu = g * s
            ggu[:, 0:FFD] = (gh * u * s * (1.0 + g * (1.0 - s))).astype(BF)
            ggu[:, FFD:2 * FFD] = (gh * silu).astype(BF)
            dots = jnp.sum(gh * silu * u, axis=1, keepdims=True)
            at = iota((ROWS, FFD), 1) == (iota((ROWS, FFD), 0) >> 5)
            spot = jnp.where(at, jnp.broadcast_to(dots, (ROWS, FFD)), 0.0).astype(BF)
            o = iota((FFD, ROWS), 0)
            i2 = iota((FFD, ROWS), 1) & 31
            pick = onehot(((o & 7) < 2) & (i2 == (o >> 3) * 2 + (o & 7)))
            dbuf[...] = nn(pick, spot).reshape(4, 4, 8, FFD)

    def f32(v):
        return v.astype(F32)

    @pl.loop(0, STEPS)
    def _(t):
        def event(lag, lo=0, hi=NJ):
            def wrap(f):
                @pl.when((t - lag >= lo) & (t - lag < hi))
                def _():
                    f(t - lag)
            return wrap

        @event(0)
        def _(j):
            pack(j)
            send(Z, j=j)

            @pl.when(j == 1)
            def _():
                tables()

        @event(E1)
        def _(j):
            arrived(Z, j)
            send(A_L, A_R, j=j)

        @event(E2)
        def _(j):
            arrived(A_L, j)
            send(FA_L, j=j)
            arrived(A_R, j)
            send(FA_R, j=j)

        @event(E3)
        def _(j):
            arrived(FA_L, j)
            arrived(FA_R, j)
            send(B_L, B_R, j=j)

        @event(E4)
        def _(j):
            arrived(B_L, j)
            send(FB_L, j=j)
            arrived(B_R, j)
            send(FB_R, j=j)

        @event(R0)
        def _(j):
            @pl.when(j < NC)
            def _():
                i = pl.multiple_of(j * CH, CH)
                repack(j, nn(hid[...], wd[:, pl.ds(i, CH)]))

            @pl.when(j >= NC)
            def _():
                i = pl.multiple_of((j - NC) * CH, CH)
                repack(j, nt(ggu[...], gu[pl.ds(i, CH), :]))

            send(BO_L, BO_R, j=j)

            @pl.when(j == NC)
            def _():
                extra(dbuf.at[bopp], dbo, DBO, dev_br).start()

        @event(R1)
        def _(j):
            arrived(BO_L, j)
            qbuf[j, br, 0:2] = (f32(qbuf[j, br, 0:2]) + f32(bo[j, 0])).astype(BF)
            send(BN_L, j=j)
            arrived(BO_R, j)
            qbuf[j, bl, 2:4] = (f32(qbuf[j, bl, 2:4]) + f32(bo[j, 1])).astype(BF)
            send(BN_R, j=j)

            @pl.when(j == NC)
            def _():
                extra(dbuf.at[bopp], dbo, DBO, dev_br).wait()
                dbuf[br] = dbuf[br] + dbo[...]
                extra(dbuf.at[br], dbn.at[0], DBN_L, dev_br).start()
                extra(dbuf.at[bl], dbn.at[1], DBN_R, dev_bl).start()

        @event(R2)
        def _(j):
            arrived(BN_L, j)
            arrived(BN_R, j)
            qbuf[j, b] = (f32(qbuf[j, b]) + f32(bn[j, 0]) + f32(bn[j, 1])).astype(BF)
            send(AO_L, AO_R, j=j)

            @pl.when(j == NC)
            def _():
                extra(dbuf.at[br], dbn.at[0], DBN_L, dev_br).wait()
                extra(dbuf.at[bl], dbn.at[1], DBN_R, dev_bl).wait()
                dbuf[b] = dbuf[b] + dbn[0] + dbn[1]
                extra(dbuf.at[b, aopp], dao, DAO, dev_ar).start()

        @event(R3)
        def _(j):
            arrived(AO_L, j)
            qbuf[j, b, ar, 0] = (f32(qbuf[j, b, ar, 0]) + f32(ao[j, 0])).astype(BF)
            send(AN_L, j=j)
            arrived(AO_R, j)
            qbuf[j, b, al, 1] = (f32(qbuf[j, b, al, 1]) + f32(ao[j, 1])).astype(BF)
            send(AN_R, j=j)

            @pl.when(j == NC)
            def _():
                extra(dbuf.at[b, aopp], dao, DAO, dev_ar).wait()
                dbuf[b, ar] = dbuf[b, ar] + dao[...]
                extra(dbuf.at[b, ar], dan.at[0], DAN_L, dev_ar).start()
                extra(dbuf.at[b, al], dan.at[1], DAN_R, dev_al).start()

        @event(R4)
        def _(j):
            arrived(AN_L, j)
            arrived(AN_R, j)
            fbuf[j] = (f32(qbuf[j, b, a]) + f32(an[j, 0]) + f32(an[j, 1])).astype(BF)
            send(FIN0, FIN1, j=j)

            @pl.when(j == NC)
            def _():
                extra(dbuf.at[b, ar], dan.at[0], DAN_L, dev_ar).wait()
                extra(dbuf.at[b, al], dan.at[1], DAN_R, dev_al).wait()
                dfin[...] = dbuf[b, a] + dan[0] + dan[1]
                extra(dfin, dz, DZ, dev_z).start()

        @event(R5)
        def _(j):
            arrived(FIN0, j)
            arrived(FIN1, j)
            v = jnp.concatenate(
                [fin[j, h, :, c * FFD:(c + 1) * FFD] for h in range(2) for c in range(5)], axis=0
            )
            u = nn(sel[...], v).astype(BF)
            for k in range(8):
                ubuf[j, :, k * FFD:(k + 1) * FFD] = u[k * 32:(k + 1) * 32]
            pltpu.make_async_copy(ubuf.at[j], u_out.at[j], usem.at[j]).start()
            sent(BO_L, BO_R, BN_L, BN_R, AO_L, AO_R, AN_L, AN_R, FIN0, FIN1, j=j)

            @pl.when(j == NC)
            def _():
                extra(dfin, dz, DZ, dev_z).wait()
                la = iota((8, FFD), 1)
                mine = jnp.where(la < 5, dfin[...], dz[...]).T
                r16 = iota((16, TOK), 0)
                s16 = jnp.where(r16 < 5, r16, r16 - 5) * 2
                total = jnp.zeros((16, TOK), F32)
                for par in range(2):
                    hit0 = jnp.where(rk[1, 0, 0:1] == s16 + par, 1.0, 0.0)
                    hit1 = jnp.where(rk[1, 1, 0:1] == s16 + par, 1.0, 0.0)
                    hit = jnp.where(r16 < 5, hit0, hit1)
                    total = total + hit * mine[0:16, par:par + 1]
                d0 = jnp.sum(jnp.where(r16 < 5, total, 0.0), axis=0, keepdims=True)
                d1 = jnp.sum(jnp.where((r16 >= 5) & (r16 < 10), total, 0.0), axis=0, keepdims=True)
                which = ids[1]
                ggb[...] = jnp.where(which == zlo, d0, 0.0) + jnp.where(
                    which == 1 - zlo, d1, 0.0
                )
                pltpu.make_async_copy(ggb, gg_out, osem).start()

        @event(E5)
        def _(j):
            @pl.when(j == 0)
            def _():
                saved()

            arrived(FB_L, j)
            arrived(FB_R, j)
            unpack(j)

            @pl.when(j < NC)
            def _():
                forward_rows(j)

            @pl.when(j >= NC)
            def _():
                backward_rows(j)

            sent(Z, A_L, A_R, FA_L, FA_R, B_L, B_R, FB_L, FB_R, j=j)

    for c in wt_copies:
        c.wait()
    pltpu.make_async_copy(ggb, gg_out, osem).wait()
    for j in range(NJ):
        pltpu.make_async_copy(ubuf.at[j], u_out.at[j], usem.at[j]).wait()


def relay(*args):
    any_spec = pl.BlockSpec(memory_space=pl.ANY)
    vmem = pltpu.VMEM
    return pl.pallas_call(
        relay_kernel,
        out_shape=(
            jax.ShapeDtypeStruct((NJ, 32, CH), BF),
            jax.ShapeDtypeStruct((2, 32, TOK), F32),
            jax.ShapeDtypeStruct((8, TOK), F32),
        ),
        in_specs=[any_spec] * 11,
        out_specs=(any_spec,) * 3,
        scratch_shapes=[
            vmem((NJ, TOK, CH), BF),
            vmem((D, 2 * FFD), BF),
            vmem((FFD, D), BF),
            vmem((2, 8, TOK), jnp.int32),
            vmem((2, 8, TOK), F32),
            vmem((ROWS, 2 * FFD), BF),
            vmem((ROWS, 2 * FFD), F32),
            vmem((NJ, 4, 4, 2, SUB, PW), BF),
            vmem((NJ, SUB, PW), BF),
            vmem((NJ, 4, 4, 2, SUB, PW), BF),
            vmem((NJ, 2, 2, 2, SUB, PW), BF),
            vmem((NJ, 2, 4, 2, SUB, PW), BF),
            vmem((NJ, 2, SUB, PW), BF),
            vmem((NJ, 2, 2, SUB, PW), BF),
            vmem((NJ, 2, SUB, PW), BF),
            vmem((NJ, 2, SUB, PW), BF),
            vmem((NJ, 32, CH), BF),
            vmem((256, 160), BF),
            vmem((2, 160, TOK), BF),
            vmem((2, 2, 8, TOK), jnp.int32),
            vmem((2, 32, TOK), F32),
            vmem((256, 256), BF),
            vmem((256, 256), BF),
            vmem((ROWS, CH), BF),
            vmem((ROWS, 2 * FFD), F32),
            vmem((ROWS, FFD), F32),
            vmem((ROWS, FFD), BF),
            vmem((ROWS, 2 * FFD), BF),
            vmem((4, 4, 8, FFD), F32),
            vmem((4, 8, FFD), F32),
            vmem((2, 4, 8, FFD), F32),
            vmem((8, FFD), F32),
            vmem((2, 8, FFD), F32),
            vmem((8, FFD), F32),
            vmem((8, FFD), F32),
            vmem((8, TOK), F32),
            pltpu.SemaphoreType.DMA((NK, NJ)),
            pltpu.SemaphoreType.DMA((NK, NJ)),
            pltpu.SemaphoreType.DMA((NX,)),
            pltpu.SemaphoreType.DMA((NX,)),
            pltpu.SemaphoreType.DMA((NJ + 9,)),
            pltpu.SemaphoreType.DMA,
            pltpu.SemaphoreType.DMA((NJ,)),
        ],
        compiler_params=pltpu.CompilerParams(
            collective_id=0, has_side_effects=True, vmem_limit_bytes=62 * 2**20
        ),
        name="relay",
    )(*args)


def spread_kernel(uf, ub, wt, gg, next_ref, prev_ref, gg_ref, lhs):
    @pl.when(pl.program_id(0) == 0)
    def _():
        gg_ref[0] = gg[...]
        for p in range(2):
            w = wt[p].T
            hi = w.astype(BF)
            lhs[p, :, 0:32] = hi
            lhs[p, :, 32:64] = (w - hi.astype(F32)).astype(BF)

    for p, (src, dst) in enumerate(((uf, next_ref), (ub, prev_ref))):
        both = jnp.concatenate([src[0], src[0]], axis=0)
        dst[0] = nn(lhs[p], both).astype(BF)


def dense(u, wt, gg):
    return pl.pallas_call(
        spread_kernel,
        grid=(NC,),
        out_shape=(
            jax.ShapeDtypeStruct((1, TOK, D), BF),
            jax.ShapeDtypeStruct((1, TOK, D), BF),
            jax.ShapeDtypeStruct((1, 8, TOK), F32),
        ),
        in_specs=[
            pl.BlockSpec((1, 32, CH), lambda i: (i, 0, 0)),
            pl.BlockSpec((1, 32, CH), lambda i: (i + NC, 0, 0)),
            pl.BlockSpec((2, 32, TOK), lambda i: (0, 0, 0)),
            pl.BlockSpec((8, TOK), lambda i: (0, 0)),
        ],
        out_specs=(
            pl.BlockSpec((1, TOK, CH), lambda i: (0, 0, i)),
            pl.BlockSpec((1, TOK, CH), lambda i: (0, 0, i)),
            pl.BlockSpec((1, 8, TOK), lambda i: (0, 0, 0)),
        ),
        scratch_shapes=[pltpu.VMEM((2, TOK, 64), BF)],
        name="dense",
    )(u, u, wt, gg)


def body(*args):
    args = args[:2] + tuple(jnp.swapaxes(x, 1, 2) for x in args[2:6]) + args[6:]
    u, wt, gg = relay(*args)
    nxt, prv, grad = dense(u, wt, gg)
    return nxt, prv, jnp.swapaxes(grad, 1, 2)


def solution(mesh):
    rows = P("section", "expert", None)
    cols = P("section", None, "expert")
    return jax.shard_map(
        body,
        mesh=mesh,
        in_specs=(rows,) * 6 + (cols, cols, rows, cols, cols),
        out_specs=(rows,) * 3,
        check_vma=False,
    )
```

```python
import jax
import jax.numpy as jnp
from jax import lax
from jax.experimental import pallas as pl
from jax.experimental.pallas import tpu as pltpu
from jax.sharding import PartitionSpec as P

MESH = pl.DeviceIdType.MESH
BF = jnp.bfloat16
F32 = jnp.float32

D = 7168
NC = 7
CH = D // NC
NJ = 2 * NC
TOK = 128
FFD = 128
SUB = 16
PW = 640
ROWS = 320

(Z, A_L, A_R, F_L, F_R, G_L, G_R, B_L, B_R, FB_L, FB_R) = range(11)
(BO_L, BO_R, BN_L, BN_R, AN_L, AN_R, AO_L, AO_R, AF_L, AF_R, FIN0, FIN1) = range(11, 23)
NK = 23
(DBO, DBN_L, DBN_R, DAO, DAN_L, DAN_R, DZ, WT0, WT1) = range(9)
(PX_G, PX_U, HID_L, HID_R, GH_L, GH_R, GG_G, GG_U) = range(9, 17)
NX = 17
(W_G, W_U, W_DL, W_DR) = range(4)

HF = CH // 2
CUT = 384

E1, E2, E3, E4, E5 = 1, 3, 5, 7, 9
X1 = E5 + NC + 1
X2 = X1 + 2
R0 = E5 + 11
X3 = E5 + NJ + 1
X4 = X3 + 2
R1, R2, R3, R4, R5 = R0 + 2, R0 + 4, R0 + 6, R0 + 8, R0 + 10
STEPS = NJ + R5


def iota(shape, dim):
    return lax.broadcasted_iota(jnp.int32, shape, dim)


def onehot(cond):
    return jnp.where(cond, 1.0, 0.0).astype(BF)


def nn(a, b):
    return jnp.dot(a, b, preferred_element_type=F32)


def nt(a, b):
    return lax.dot_general(a, b, (((1,), (1,)), ((), ())), preferred_element_type=F32)


def relay_kernel(
    act, cot, fids, fgates, bids, bgates, gw, uw, dw, gpre, upre,
    u_out, wt_out, gg_out,
    tok, gu, wd, ids, gates, pre, pref, obuf, zbuf, zin, sbuf, gbuf, fst0, fst1,
    qbuf, bo, bn, an, ao, afs0, afs1, fbuf, fin, ubuf, sel,
    lhs, rk, wts, perm_u, perm_p, xbuf, acc, accb, px, prx, hid, hx, hcat, ghx, ghr, gga, ggx, ggu,
    dbuf, dbo, dbn, dao, dan, dfin, dz, ggb,
    ssem, rsem, wss, wrs, xs, xr, lsem, wsem, osem, usem,
):
    sec = lax.axis_index("section")
    exp = lax.axis_index("expert")
    core = lax.rem(sec, 2)
    zlo = exp // 16
    cx = lax.rem(exp // 4, 4)
    cy = lax.rem(exp, 4)
    a = cx * (1 - core) + cy * core
    b = cy * (1 - core) + cx * core
    half = lax.rem(a, 2)
    al, ar, aopp = lax.rem(a + 3, 4), lax.rem(a + 1, 4), lax.rem(a + 2, 4)
    bl, br, bopp = lax.rem(b + 3, 4), lax.rem(b + 1, 4), lax.rem(b + 2, 4)

    def plane(ap, bp):
        return zlo * 16 + ap * (4 - 3 * core) + bp * (1 + 3 * core)

    partner = exp + 16 - 32 * zlo
    dev_al, dev_ar = {"expert": plane(al, b)}, {"expert": plane(ar, b)}
    dev_bl, dev_br = {"expert": plane(a, bl)}, {"expert": plane(a, br)}
    dev_p1 = {"expert": plane(a + 1 - 2 * half, b)}
    dev_p2 = {"expert": plane(lax.rem(a + 3 + 2 * half, 4), b)}
    dev_z = {"expert": partner}
    nxt, prv = lax.rem(sec + 1, 8), lax.rem(sec + 7, 8)

    def load(src, dst, k):
        return pltpu.make_async_copy(src, dst, lsem.at[k])

    small = [
        load(fids.at[0], ids.at[0], NJ),
        load(bids.at[0], ids.at[1], NJ + 1),
        load(fgates.at[0], gates.at[0], NJ + 2),
        load(bgates.at[0], gates.at[1], NJ + 3),
    ]
    pres = [
        load(gpre.at[0], pre.at[:, pl.ds(0, FFD)], NJ + 4),
        load(upre.at[0], pre.at[:, pl.ds(FFD, FFD)], NJ + 5),
    ]
    toks = []
    for j in range(NJ):
        src = act if j < NC else cot
        toks.append(load(src.at[0, :, pl.ds((j % NC) * CH, CH)], tok.at[j], j))

    def feats(i, h):
        return pl.ds(pl.multiple_of(i * CH + h * HF, HF), HF)

    def own_weight(k, i):
        src = (gw, uw, dw)[k]
        if k < 2:
            src = src.at[0, feats(i, half), :]
            dst = gu.at[i, :, pl.ds(2 * k * FFD, FFD)]
        else:
            src = src.at[0, :, feats(i, half)]
            dst = wd.at[i, pl.ds(0, FFD), :]
        return pltpu.make_async_copy(src, dst, wsem.at[k, i])

    for c in small:
        c.start()
    for c in toks[:NC]:
        c.start()
    for i in range(NC):
        own_weight(0, i).start()
        own_weight(1, i).start()
    for c in toks[NC:]:
        c.start()
    for i in range(NC):
        own_weight(2, i).start()
    for c in pres:
        c.start()

    barrier = pltpu.get_barrier_semaphore()
    peers = [dev_al, dev_ar, dev_bl, dev_br, dev_z]
    for s in (nxt, prv):
        peers.append({"section": s, "expert": exp})
        peers.append({"section": s, "expert": partner})
    for dev in peers:
        pl.semaphore_signal(barrier, inc=1, device_id=dev, device_id_type=MESH)

    for c in small:
        c.wait()
    upper = onehot(iota((TOK, TOK), 0) <= iota((TOK, TOK), 1))
    slot16 = iota((16, TOK), 0)
    row160 = iota((160, TOK), 0)
    row_slot = (jnp.where(row160 >= 80, row160 - 80, row160) >> 4) * 2 + ((row160 >> 2) & 1)
    for p in range(2):
        ranks = []
        for h in range(2):
            e = zlo if h == 0 else 1 - zlo
            match = ids[p] == e
            routed = jnp.max(jnp.where(match, 1.0, 0.0), axis=0, keepdims=True)
            w = jnp.sum(jnp.where(match, gates[p], 0.0), axis=0, keepdims=True)
            count = nn(jnp.broadcast_to(routed, (8, TOK)).astype(BF), upper)
            rank = jnp.where(routed > 0.5, count.astype(jnp.int32) - 1, -1)
            rk[p, h] = rank
            wts[p, h * 16:h * 16 + 16] = jnp.where(slot16 == rank[0:1], w, 0.0)
            ranks.append(rank[0:1])
        low = jnp.where(row_slot == ranks[0], 1.0, 0.0)
        high = jnp.where(row_slot == ranks[1], 1.0, 0.0)
        lhs[p] = jnp.where(row160 < 80, low, high).astype(BF)
    pl.semaphore_wait(barrier, len(peers))

    def extra(src, dst, k, dev):
        return pltpu.make_async_remote_copy(
            src_ref=src, dst_ref=dst, send_sem=xs.at[k], recv_sem=xr.at[k],
            device_id=dev, device_id_type=MESH,
        )

    wt_copies = [
        extra(wts.at[0], wt_out.at[0], WT0, {"section": nxt, "expert": exp}),
        extra(wts.at[1], wt_out.at[1], WT1, {"section": prv, "expert": exp}),
    ]
    for c in wt_copies:
        c.start()

    def weight(k, i):
        other = 1 - half
        if k == W_G:
            src, dst, dev = gw.at[0, feats(i, other), :], gu.at[i, :, pl.ds(FFD, FFD)], dev_p1
        elif k == W_U:
            src, dst, dev = uw.at[0, feats(i, other), :], gu.at[i, :, pl.ds(3 * FFD, FFD)], dev_p2
        elif k == W_DL:
            src = dw.at[0, pl.ds(64, 64), feats(i, other)]
            dst, dev = wd.at[i, pl.ds(192, 64), :], dev_ar
        else:
            src = dw.at[0, pl.ds(0, 64), feats(i, other)]
            dst, dev = wd.at[i, pl.ds(128, 64), :], dev_al
        return pltpu.make_async_remote_copy(
            src_ref=src, dst_ref=dst, send_sem=wss.at[k, i], recv_sem=wrs.at[k, i],
            device_id=dev, device_id_type=MESH,
        )

    def ring(src, dst, k, j, dev):
        return pltpu.make_async_remote_copy(
            src_ref=src, dst_ref=dst, send_sem=ssem.at[k, j], recv_sem=rsem.at[k, j],
            device_id=dev, device_id_type=MESH,
        )

    lo, hi = pl.ds(0, CUT), pl.ds(CUT, PW - CUT)

    def out(k, j):
        if k == Z:
            return ring(zbuf.at[j], zin.at[j], k, j, dev_z)
        if k == A_L:
            return ring(sbuf.at[j], gbuf.at[j, b, a], k, j, dev_ar)
        if k == A_R:
            return ring(sbuf.at[j], gbuf.at[j, b, a], k, j, dev_al)
        if k == F_L:
            return ring(gbuf.at[j, b, a, :, lo], fst0.at[j], k, j, dev_ar)
        if k == F_R:
            return ring(gbuf.at[j, b, a, :, hi], fst1.at[j], k, j, dev_al)
        if k == G_L:
            return ring(fst0.at[j], gbuf.at[j, b, al, :, lo], k, j, dev_ar)
        if k == G_R:
            return ring(fst1.at[j], gbuf.at[j, b, ar, :, hi], k, j, dev_al)
        if k == B_L:
            return ring(gbuf.at[j, b], gbuf.at[j, b], k, j, dev_br)
        if k == B_R:
            return ring(gbuf.at[j, b], gbuf.at[j, b], k, j, dev_bl)
        if k == FB_L:
            two = gbuf.at[j, bl, pl.ds(0, 2)]
            return ring(two, two, k, j, dev_br)
        if k == FB_R:
            two = gbuf.at[j, br, pl.ds(2, 2)]
            return ring(two, two, k, j, dev_bl)
        if k == BO_L:
            return ring(qbuf.at[j, bopp, pl.ds(0, 2)], bo.at[j, 0], k, j, dev_br)
        if k == BO_R:
            return ring(qbuf.at[j, bopp, pl.ds(2, 2)], bo.at[j, 1], k, j, dev_bl)
        if k == BN_L:
            return ring(qbuf.at[j, br], bn.at[j, 0], k, j, dev_br)
        if k == BN_R:
            return ring(qbuf.at[j, bl], bn.at[j, 1], k, j, dev_bl)
        if k == AN_L:
            return ring(qbuf.at[j, b, ar], an.at[j, 0], k, j, dev_ar)
        if k == AN_R:
            return ring(qbuf.at[j, b, al], an.at[j, 1], k, j, dev_al)
        if k == AO_L:
            return ring(qbuf.at[j, b, aopp, :, lo], afs0.at[j], k, j, dev_ar)
        if k == AO_R:
            return ring(qbuf.at[j, b, aopp, :, hi], afs1.at[j], k, j, dev_al)
        if k == AF_L:
            return ring(afs0.at[j], ao.at[j, :, lo], k, j, dev_ar)
        if k == AF_R:
            return ring(afs1.at[j], ao.at[j, :, hi], k, j, dev_al)
        to = jnp.where(j < NC, nxt, prv)
        h = k - FIN0
        dev = {"section": to, "expert": exp if h == 0 else partner}
        return ring(fbuf.at[j, h], fin.at[j, h], k, j, dev)

    def arrived(k, j):
        dst = {
            Z: lambda: zin.at[j],
            A_L: lambda: gbuf.at[j, b, al],
            A_R: lambda: gbuf.at[j, b, ar],
            F_L: lambda: fst0.at[j],
            F_R: lambda: fst1.at[j],
            G_L: lambda: gbuf.at[j, b, aopp, :, lo],
            G_R: lambda: gbuf.at[j, b, aopp, :, hi],
            B_L: lambda: gbuf.at[j, bl],
            B_R: lambda: gbuf.at[j, br],
            FB_L: lambda: gbuf.at[j, bopp, pl.ds(0, 2)],
            FB_R: lambda: gbuf.at[j, bopp, pl.ds(2, 2)],
            BO_L: lambda: bo.at[j, 0],
            BO_R: lambda: bo.at[j, 1],
            BN_L: lambda: bn.at[j, 0],
            BN_R: lambda: bn.at[j, 1],
            AN_L: lambda: an.at[j, 0],
            AN_R: lambda: an.at[j, 1],
            AO_L: lambda: afs0.at[j],
            AO_R: lambda: afs1.at[j],
            AF_L: lambda: ao.at[j, :, lo],
            AF_R: lambda: ao.at[j, :, hi],
            FIN0: lambda: fin.at[j, 0],
            FIN1: lambda: fin.at[j, 1],
        }[k]()
        ring(dst, dst, k, j, dev_z).wait_recv()

    def send(*kinds, j):
        for k in kinds:
            out(k, j).start()

    def sent(*kinds, j):
        for k in kinds:
            out(k, j).wait_send()

    def f32(v):
        return v.astype(F32)

    r16 = iota((SUB, FFD), 0)
    row_k = ((r16 >> 3) << 2) | (r16 & 3)

    def pack(j):
        p = j // NC
        load(act.at[0, :, pl.ds(0, CH)], tok.at[j], j).wait()
        y = nn(lhs[p], tok[j])
        for h in range(2):
            for c in range(5):
                r = (h * 5 + c) * SUB
                v = y[r:r + SUB, 0:FFD]
                for k in range(1, 8):
                    v = jnp.where(row_k == k, y[r:r + SUB, k * FFD:(k + 1) * FFD], v)
                if h == 0:
                    obuf[j, :, c * FFD:(c + 1) * FFD] = v.astype(BF)
                else:
                    zbuf[j, :, c * FFD:(c + 1) * FFD] = v.astype(BF)

    def by_half(j):
        o, z = f32(obuf[j]), f32(zin[j])
        first = jnp.concatenate([o[0:8], z[0:8]], axis=0)
        second = jnp.concatenate([o[8:16], z[8:16]], axis=0)
        gbuf[j, b, a] = jnp.where(half == 0, first, second).astype(BF)
        sbuf[j] = jnp.where(half == 0, second, first).astype(BF)

    def tables():
        o = iota((256, 256), 0)
        i = iota((256, 256), 1)
        perm_u[...] = onehot(i == ((o & 63) >> 2) * 16 + (o & 3) * 4 + (o >> 6))
        perm_p[...] = onehot(o == ((i & 63) >> 2) * 16 + (i & 3) * 4 + (i >> 6))
        o = iota((256, 160), 0)
        v = iota((256, 160), 1)
        h = jnp.where(v >= 80, 1, 0)
        slot = h * 16 + ((v - 80 * h) >> 4) * 2 + ((v >> 2) & 1)
        k = (((v >> 3) & 1) << 2) | (v & 3)
        sel[...] = onehot((k == (o >> 5)) & ((o & 31) == slot))

    def saved():
        for c in pres:
            c.wait()
        i = iota((ROWS, ROWS), 0)
        h = (i >> 1) & 1
        bp = (i >> 4) & 3
        ap = (i >> 2) & 3
        xy = ap * (4 - 3 * core) + bp * (1 + 3 * core)
        pln = zlo + h - 2 * zlo * h
        src = (pln * 16 + xy) * 10 + (i >> 6) * 2 + (i & 1)
        pref[...] = nn(onehot(iota((ROWS, ROWS), 1) == src), pre[...])

    def unpack(j):
        r = nn(perm_u[...], gbuf[j].reshape(256, PW)).astype(BF)
        for c in range(5):
            for k in range(4):
                xbuf[c * 64:(c + 1) * 64, k * FFD:(k + 1) * FFD] = (
                    r[k * 64:(k + 1) * 64, c * FFD:(c + 1) * FFD]
                )

    def repack(j, o):
        o = o.astype(BF)
        cols = []
        for c in range(5):
            cols.append(
                jnp.concatenate(
                    [o[c * 64:(c + 1) * 64, k * FFD:(k + 1) * FFD] for k in range(4)], axis=0
                )
            )
        q = nn(perm_p[...], jnp.concatenate(cols, axis=1)).astype(BF)
        qbuf[j] = q.reshape(4, 4, SUB, PW)

    def px_copies():
        return [
            extra(px.at[0], prx.at[0], PX_G, dev_p1),
            extra(px.at[1], prx.at[1], PX_U, dev_p2),
        ]

    def hid_copies():
        return [
            extra(hid, hx.at[0], HID_L, dev_ar),
            extra(hid, hx.at[1], HID_R, dev_al),
        ]

    def gh_copies():
        return [
            extra(ghx, ghr.at[0], GH_L, dev_ar),
            extra(ghx, ghr.at[1], GH_R, dev_al),
        ]

    def gg_copies():
        return [
            extra(gga.at[0], ggx.at[0], GG_G, dev_p1),
            extra(gga.at[1], ggx.at[1], GG_U, dev_p2),
        ]

    def forward_rows(i):
        own_weight(0, i).wait()
        own_weight(1, i).wait()
        weight(W_G, i).wait()
        weight(W_U, i).wait()

        @pl.when(i == 0)
        def _():
            acc[...] = nn(xbuf[...], gu[i])

        @pl.when(i > 0)
        def _():
            acc[...] += nn(xbuf[...], gu[i])

        @pl.when(i == NC - 1)
        def _():
            px[0] = acc[:, FFD:2 * FFD].astype(BF)
            px[1] = acc[:, 3 * FFD:4 * FFD].astype(BF)
            for c in px_copies():
                c.start()

    def backward_rows(i):
        own_weight(2, i).wait()
        weight(W_DL, i).wait()
        weight(W_DR, i).wait()

        @pl.when(i == 0)
        def _():
            accb[...] = nt(xbuf[...], wd[i])

        @pl.when(i > 0)
        def _():
            accb[...] += nt(xbuf[...], wd[i])

        @pl.when(i == NC - 1)
        def _():
            ghx[...] = accb[:, FFD:2 * FFD].astype(BF)
            for c in gh_copies():
                c.start()

    left64 = iota((ROWS, FFD), 1) < 64

    def hidden_own():
        for c in px_copies():
            c.wait()
        g = acc[:, 0:FFD] + f32(prx[0])
        u = acc[:, 2 * FFD:3 * FFD] + f32(prx[1])
        hid[...] = (g / (1.0 + jnp.exp(-g)) * u).astype(BF)
        for c in hid_copies():
            c.start()

    def hidden_all():
        for c in hid_copies():
            c.wait()
        hcat[:, 0:FFD] = hid[...]
        hcat[:, FFD:2 * FFD] = jnp.where(left64, f32(hx[1]), f32(hx[0])).astype(BF)

    def grads_own():
        for c in gh_copies():
            c.wait()
        gh = accb[:, 0:FFD] + jnp.where(left64, f32(ghr[0]), f32(ghr[1]))
        g = pref[:, 0:FFD]
        u = pref[:, FFD:2 * FFD]
        s = 1.0 / (1.0 + jnp.exp(-g))
        silu = g * s
        gga[0] = (gh * u * s * (1.0 + g * (1.0 - s))).astype(BF)
        gga[1] = (gh * silu).astype(BF)
        for c in gg_copies():
            c.start()
        dots = jnp.sum(gh * silu * u, axis=1, keepdims=True)
        at = iota((ROWS, FFD), 1) == (iota((ROWS, FFD), 0) >> 6)
        spot = jnp.where(at, jnp.broadcast_to(dots, (ROWS, FFD)), 0.0).astype(BF)
        o = iota((FFD, ROWS), 0)
        i2 = iota((FFD, ROWS), 1) & 63
        pick = onehot(((o & 7) < 4) & (i2 == (o >> 3) * 4 + (o & 7)))
        dbuf[...] = nn(pick, spot).reshape(4, 4, 8, FFD)

    def grads_all():
        for c in gg_copies():
            c.wait()
        ggu[:, 0:FFD] = gga[0]
        ggu[:, FFD:2 * FFD] = ggx[0]
        ggu[:, 2 * FFD:3 * FFD] = gga[1]
        ggu[:, 3 * FFD:4 * FFD] = ggx[1]

    @pl.loop(0, STEPS)
    def _(t):
        def event(lag, lo=0, hi=NJ):
            def wrap(f):
                @pl.when((t - lag >= lo) & (t - lag < hi))
                def _():
                    f(t - lag)
            return wrap

        @event(0)
        def _(j):
            pack(j)
            send(Z, j=j)

            @pl.when(j == 1)
            def _():
                tables()

        @event(E1)
        def _(j):
            arrived(Z, j)
            by_half(j)
            send(A_L, A_R, F_L, F_R, j=j)

            @pl.when(j < NC)
            def _():
                weight(W_G, j).start()
                weight(W_U, j).start()

            @pl.when(j >= NC)
            def _():
                weight(W_DL, j - NC).start()
                weight(W_DR, j - NC).start()

        @event(E2)
        def _(j):
            arrived(F_L, j)
            send(G_L, j=j)
            arrived(F_R, j)
            send(G_R, j=j)

        @event(E3)
        def _(j):
            arrived(A_L, j)
            arrived(A_R, j)
            arrived(G_L, j)
            arrived(G_R, j)
            send(B_L, B_R, j=j)

        @event(E4)
        def _(j):
            arrived(B_L, j)
            send(FB_L, j=j)
            arrived(B_R, j)
            send(FB_R, j=j)

        for step, act_now in ((X1, hidden_own), (X2, hidden_all), (X3, grads_own), (X4, grads_all)):
            pl.when(t == step)(act_now)

        @event(R0)
        def _(j):
            @pl.when(j < NC)
            def _():
                repack(j, nn(hcat[...], wd[j]))

            @pl.when(j >= NC)
            def _():
                repack(j, nt(ggu[...], gu[j - NC]))

            send(BO_L, BO_R, j=j)

            @pl.when(j == NC)
            def _():
                extra(dbuf.at[bopp], dbo, DBO, dev_br).start()

        @event(R1)
        def _(j):
            arrived(BO_L, j)
            qbuf[j, br, 0:2] = (f32(qbuf[j, br, 0:2]) + f32(bo[j, 0])).astype(BF)
            send(BN_L, j=j)
            arrived(BO_R, j)
            qbuf[j, bl, 2:4] = (f32(qbuf[j, bl, 2:4]) + f32(bo[j, 1])).astype(BF)
            send(BN_R, j=j)

            @pl.when(j == NC)
            def _():
                extra(dbuf.at[bopp], dbo, DBO, dev_br).wait()
                dbuf[br] = dbuf[br] + dbo[...]
                extra(dbuf.at[br], dbn.at[0], DBN_L, dev_br).start()
                extra(dbuf.at[bl], dbn.at[1], DBN_R, dev_bl).start()

        @event(R2)
        def _(j):
            arrived(BN_L, j)
            arrived(BN_R, j)
            qbuf[j, b] = (f32(qbuf[j, b]) + f32(bn[j, 0]) + f32(bn[j, 1])).astype(BF)
            send(AO_L, AO_R, AN_L, AN_R, j=j)

            @pl.when(j == NC)
            def _():
                extra(dbuf.at[br], dbn.at[0], DBN_L, dev_br).wait()
                extra(dbuf.at[bl], dbn.at[1], DBN_R, dev_bl).wait()
                dbuf[b] = dbuf[b] + dbn[0] + dbn[1]
                extra(dbuf.at[b, aopp], dao, DAO, dev_ar).start()

        @event(R3)
        def _(j):
            arrived(AO_L, j)
            send(AF_L, j=j)
            arrived(AO_R, j)
            send(AF_R, j=j)

            @pl.when(j == NC)
            def _():
                extra(dbuf.at[b, aopp], dao, DAO, dev_ar).wait()
                dbuf[b, ar] = dbuf[b, ar] + dao[...]
                extra(dbuf.at[b, ar], dan.at[0], DAN_L, dev_ar).start()
                extra(dbuf.at[b, al], dan.at[1], DAN_R, dev_al).start()

        @event(R4)
        def _(j):
            arrived(AN_L, j)
            arrived(AN_R, j)
            arrived(AF_L, j)
            arrived(AF_R, j)
            mine = f32(qbuf[j, b, a]) + f32(ao[j])
            theirs = f32(an[j, 0]) + f32(an[j, 1])
            first = jnp.where(half == 0, mine, theirs)
            second = jnp.where(half == 0, theirs, mine)
            for h in range(2):
                r = h * 8
                fbuf[j, h] = jnp.concatenate([first[r:r + 8], second[r:r + 8]], axis=0).astype(BF)
            send(FIN0, FIN1, j=j)

            @pl.when(j == NC)
            def _():
                extra(dbuf.at[b, ar], dan.at[0], DAN_L, dev_ar).wait()
                extra(dbuf.at[b, al], dan.at[1], DAN_R, dev_al).wait()
                dfin[...] = dbuf[b, a] + dan[0] + dan[1]
                extra(dfin, dz, DZ, dev_z).start()

        @event(R5)
        def _(j):
            arrived(FIN0, j)
            arrived(FIN1, j)
            v = jnp.concatenate(
                [fin[j, h, :, c * FFD:(c + 1) * FFD] for h in range(2) for c in range(5)], axis=0
            )
            u = nn(sel[...], v).astype(BF)
            for k in range(8):
                ubuf[j, :, k * FFD:(k + 1) * FFD] = u[k * 32:(k + 1) * 32]
            pltpu.make_async_copy(ubuf.at[j], u_out.at[j], usem.at[j]).start()
            sent(
                BO_L, BO_R, BN_L, BN_R, AN_L, AN_R, AO_L, AO_R, AF_L, AF_R, FIN0, FIN1, j=j
            )

            @pl.when(j == NC)
            def _():
                extra(dfin, dz, DZ, dev_z).wait()
                la = iota((8, FFD), 0)
                mine = jnp.where(la < 2, dfin[...], dz[...]).T
                c8 = iota((8, TOK), 0)
                which = ids[1]
                total = jnp.zeros((8, TOK), F32)
                for h in range(2):
                    d = jnp.zeros((8, TOK), F32)
                    for par in range(2):
                        hit = jnp.where((rk[1, h, 0:1] == c8 * 2 + par) & (c8 < 5), 1.0, 0.0)
                        d = d + hit * mine[0:8, h * 2 + par:h * 2 + par + 1]
                    d = jnp.sum(d, axis=0, keepdims=True)
                    e = zlo if h == 0 else 1 - zlo
                    total = total + jnp.where(which == e, d, 0.0)
                ggb[...] = total
                pltpu.make_async_copy(ggb, gg_out, osem).start()

        @event(E5)
        def _(j):
            @pl.when(j == 0)
            def _():
                saved()

            arrived(FB_L, j)
            arrived(FB_R, j)
            unpack(j)

            @pl.when(j < NC)
            def _():
                forward_rows(j)

            @pl.when(j >= NC)
            def _():
                backward_rows(j - NC)

            sent(Z, A_L, A_R, F_L, F_R, G_L, G_R, B_L, B_R, FB_L, FB_R, j=j)

    for c in wt_copies:
        c.wait()
    pltpu.make_async_copy(ggb, gg_out, osem).wait()
    for j in range(NJ):
        pltpu.make_async_copy(ubuf.at[j], u_out.at[j], usem.at[j]).wait()


def relay(*args):
    any_spec = pl.BlockSpec(memory_space=pl.ANY)
    vmem = pltpu.VMEM
    dma = pltpu.SemaphoreType.DMA
    return pl.pallas_call(
        relay_kernel,
        out_shape=(
            jax.ShapeDtypeStruct((NJ, 32, CH), BF),
            jax.ShapeDtypeStruct((2, 32, TOK), F32),
            jax.ShapeDtypeStruct((8, TOK), F32),
        ),
        in_specs=[any_spec] * 11,
        out_specs=(any_spec,) * 3,
        scratch_shapes=[
            vmem((NJ, TOK, CH), BF),
            vmem((NC, HF, 4 * FFD), BF),
            vmem((NC, 2 * FFD, HF), BF),
            vmem((2, 8, TOK), jnp.int32),
            vmem((2, 8, TOK), F32),
            vmem((ROWS, 2 * FFD), BF),
            vmem((ROWS, 2 * FFD), F32),
            vmem((NJ, SUB, PW), BF),
            vmem((NJ, SUB, PW), BF),
            vmem((NJ, SUB, PW), BF),
            vmem((NJ, SUB, PW), BF),
            vmem((NJ, 4, 4, SUB, PW), BF),
            vmem((NJ, SUB, CUT), BF),
            vmem((NJ, SUB, PW - CUT), BF),
            vmem((NJ, 4, 4, SUB, PW), BF),
            vmem((NJ, 2, 2, SUB, PW), BF),
            vmem((NJ, 2, 4, SUB, PW), BF),
            vmem((NJ, 2, SUB, PW), BF),
            vmem((NJ, SUB, PW), BF),
            vmem((NJ, SUB, CUT), BF),
            vmem((NJ, SUB, PW - CUT), BF),
            vmem((NJ, 2, SUB, PW), BF),
            vmem((NJ, 2, SUB, PW), BF),
            vmem((NJ, 32, CH), BF),
            vmem((256, 160), BF),
            vmem((2, 160, TOK), BF),
            vmem((2, 2, 8, TOK), jnp.int32),
            vmem((2, 32, TOK), F32),
            vmem((256, 256), BF),
            vmem((256, 256), BF),
            vmem((ROWS, HF), BF),
            vmem((ROWS, 4 * FFD), F32),
            vmem((ROWS, 2 * FFD), F32),
            vmem((2, ROWS, FFD), BF),
            vmem((2, ROWS, FFD), BF),
            vmem((ROWS, FFD), BF),
            vmem((2, ROWS, FFD), BF),
            vmem((ROWS, 2 * FFD), BF),
            vmem((ROWS, FFD), BF),
            vmem((2, ROWS, FFD), BF),
            vmem((2, ROWS, FFD), BF),
            vmem((2, ROWS, FFD), BF),
            vmem((ROWS, 4 * FFD), BF),
            vmem((4, 4, 8, FFD), F32),
            vmem((4, 8, FFD), F32),
            vmem((2, 4, 8, FFD), F32),
            vmem((8, FFD), F32),
            vmem((2, 8, FFD), F32),
            vmem((8, FFD), F32),
            vmem((8, FFD), F32),
            vmem((8, TOK), F32),
            dma((NK, NJ)),
            dma((NK, NJ)),
            dma((4, NC)),
            dma((4, NC)),
            dma((NX,)),
            dma((NX,)),
            dma((NJ + 6,)),
            dma((3, NC)),
            dma,
            dma((NJ,)),
        ],
        compiler_params=pltpu.CompilerParams(
            collective_id=0, has_side_effects=True, vmem_limit_bytes=62 * 2**20
        ),
        name="relay",
    )(*args)


def spread_kernel(uf, ub, wt, gg, next_ref, prev_ref, gg_ref, lhs):
    @pl.when(pl.program_id(0) == 0)
    def _():
        gg_ref[0] = gg[...]
        for p in range(2):
            w = wt[p].T
            hi = w.astype(BF)
            lhs[p, :, 0:32] = hi
            lhs[p, :, 32:64] = (w - hi.astype(F32)).astype(BF)

    for p, (src, dst) in enumerate(((uf, next_ref), (ub, prev_ref))):
        both = jnp.concatenate([src[0], src[0]], axis=0)
        dst[0] = nn(lhs[p], both).astype(BF)


def dense(u, wt, gg):
    return pl.pallas_call(
        spread_kernel,
        grid=(NC,),
        out_shape=(
            jax.ShapeDtypeStruct((1, TOK, D), BF),
            jax.ShapeDtypeStruct((1, TOK, D), BF),
            jax.ShapeDtypeStruct((1, 8, TOK), F32),
        ),
        in_specs=[
            pl.BlockSpec((1, 32, CH), lambda i: (i, 0, 0)),
            pl.BlockSpec((1, 32, CH), lambda i: (i + NC, 0, 0)),
            pl.BlockSpec((2, 32, TOK), lambda i: (0, 0, 0)),
            pl.BlockSpec((8, TOK), lambda i: (0, 0)),
        ],
        out_specs=(
            pl.BlockSpec((1, TOK, CH), lambda i: (0, 0, i)),
            pl.BlockSpec((1, TOK, CH), lambda i: (0, 0, i)),
            pl.BlockSpec((1, 8, TOK), lambda i: (0, 0, 0)),
        ),
        scratch_shapes=[pltpu.VMEM((2, TOK, 64), BF)],
        name="dense",
    )(u, u, wt, gg)


def body(*args):
    args = args[:2] + tuple(jnp.swapaxes(x, 1, 2) for x in args[2:6]) + args[6:]
    u, wt, gg = relay(*args)
    nxt, prv, grad = dense(u, wt, gg)
    return nxt, prv, jnp.swapaxes(grad, 1, 2)


def solution(mesh):
    rows = P("section", "expert", None)
    cols = P("section", None, "expert")
    return jax.shard_map(
        body,
        mesh=mesh,
        in_specs=(rows,) * 6 + (cols, cols, rows, cols, cols),
        out_specs=(rows,) * 3,
        check_vma=False,
    )
```

```python
import jax
import jax.numpy as jnp
from jax import lax
from jax.experimental import pallas as pl
from jax.experimental.pallas import tpu as pltpu
from jax.sharding import PartitionSpec as P

MESH = pl.DeviceIdType.MESH
BF = jnp.bfloat16
F32 = jnp.float32

D = 7168
NC = 7
CH = D // NC
NJ = 2 * NC
TOK = 128
FFD = 128
SUB = 16
PW = 640
ROWS = 320

(Z, A_L, A_R, A_O, B_L, B_R, FB_L, FB_R) = range(8)
(BO_L, BO_R, BN_L, BN_R, AN_L, AN_R, AN_O, FIN0, FIN1) = range(8, 17)
(GZ, GA, GB, GFB, GBO, GBN, GAN, GFIN) = range(8)
NG = 8
GROUP = (GZ, GA, GA, GA, GB, GB, GFB, GFB, GBO, GBO, GBN, GBN, GAN, GAN, GAN, GFIN, GFIN)
BLOCKS = (1, 3, 8, 4, 4, 8, 3, 2)
SENT = (16, 17)
(DBO, DBN_L, DBN_R, DAO, DAN_L, DAN_R, DZ, WT0, WT1) = range(9)
(PX_G, PX_U, HID_L, HID_R, GH_L, GH_R, GG_G, GG_U) = range(9, 17)
NX = 17
(W_G, W_U, W_DL, W_DR) = range(4)

AHEAD = 2
HF = CH // 2

E1, E2, E3, E4 = 1, 3, 5, 7
X1 = E4 + NC + 1
X2 = X1 + 2
R0 = E4 + 11
X3 = E4 + NJ + 1
X4 = X3 + 2
R1, R2, R3, R4 = R0 + 2, R0 + 5, R0 + 8, R0 + 11
STEPS = NJ + R4


def iota(shape, dim):
    return lax.broadcasted_iota(jnp.int32, shape, dim)


def onehot(cond):
    return jnp.where(cond, 1.0, 0.0).astype(BF)


def nn(a, b):
    return jnp.dot(a, b, preferred_element_type=F32)


def nt(a, b):
    return lax.dot_general(a, b, (((1,), (1,)), ((), ())), preferred_element_type=F32)


def relay_kernel(
    act, cot, fids, fgates, bids, bgates, gw, uw, dw, gpre, upre,
    u_out, wt_out, gg_out,
    tok, gu, wd, ids, gates, pre, pref, obuf, zbuf, zin, sbuf, gbuf,
    qbuf, bo, bn, an, ao, fbuf, fin, ubuf, sel,
    lhs, rk, wts, perm_u, perm_p, xbuf, acc, accb, px, prx, hid, hx, hcat, ghx, ghr, gga, ggx, ggu,
    dbuf, dbo, dbn, dao, dan, dfin, dz, ggb, size,
    ssem, rsem, wss, wrs, xs, xr, lsem, wsem, osem, usem,
):
    sec = lax.axis_index("section")
    exp = lax.axis_index("expert")
    core = lax.rem(sec, 2)
    zlo = exp // 16
    cx = lax.rem(exp // 4, 4)
    cy = lax.rem(exp, 4)
    a = cx * (1 - core) + cy * core
    b = cy * (1 - core) + cx * core
    half = lax.rem(a, 2)
    al, ar, aopp = lax.rem(a + 3, 4), lax.rem(a + 1, 4), lax.rem(a + 2, 4)
    bl, br, bopp = lax.rem(b + 3, 4), lax.rem(b + 1, 4), lax.rem(b + 2, 4)

    def plane(ap, bp):
        return zlo * 16 + ap * (4 - 3 * core) + bp * (1 + 3 * core)

    partner = exp + 16 - 32 * zlo
    dev_al, dev_ar = {"expert": plane(al, b)}, {"expert": plane(ar, b)}
    dev_ao = {"expert": plane(aopp, b)}
    dev_bl, dev_br = {"expert": plane(a, bl)}, {"expert": plane(a, br)}
    dev_p1 = {"expert": plane(a + 1 - 2 * half, b)}
    dev_p2 = {"expert": plane(lax.rem(a + 3 + 2 * half, 4), b)}
    dev_z = {"expert": partner}
    nxt, prv = lax.rem(sec + 1, 8), lax.rem(sec + 7, 8)

    def load(src, dst, k):
        return pltpu.make_async_copy(src, dst, lsem.at[k])

    small = [
        load(fids.at[0], ids.at[0], NJ),
        load(bids.at[0], ids.at[1], NJ + 1),
        load(fgates.at[0], gates.at[0], NJ + 2),
        load(bgates.at[0], gates.at[1], NJ + 3),
    ]
    pres = [
        load(gpre.at[0], pre.at[:, pl.ds(0, FFD)], NJ + 4),
        load(upre.at[0], pre.at[:, pl.ds(FFD, FFD)], NJ + 5),
    ]
    toks = []
    for j in range(NJ):
        src = act if j < NC else cot
        toks.append(load(src.at[0, :, pl.ds((j % NC) * CH, CH)], tok.at[j], j))

    def feats(i, h):
        return pl.ds(pl.multiple_of(i * CH + h * HF, HF), HF)

    def own_weight(k, i):
        src = (gw, uw, dw)[k]
        if k < 2:
            src = src.at[0, feats(i, half), :]
            dst = gu.at[i, :, pl.ds(2 * k * FFD, FFD)]
        else:
            src = src.at[0, :, feats(i, half)]
            dst = wd.at[i, pl.ds(0, FFD), :]
        return pltpu.make_async_copy(src, dst, wsem.at[k, i])

    for c in small:
        c.start()
    for c in toks[:NC]:
        c.start()
    for i in range(NC):
        own_weight(0, i).start()
        own_weight(1, i).start()
    for c in toks[NC:]:
        c.start()
    for i in range(NC):
        own_weight(2, i).start()
    for c in pres:
        c.start()

    barrier = pltpu.get_barrier_semaphore()
    peers = [dev_al, dev_ar, dev_ao, dev_bl, dev_br, dev_z]
    for s in (nxt, prv):
        peers.append({"section": s, "expert": exp})
        peers.append({"section": s, "expert": partner})
    for dev in peers:
        pl.semaphore_signal(barrier, inc=1, device_id=dev, device_id_type=MESH)

    for c in small:
        c.wait()
    upper = onehot(iota((TOK, TOK), 0) <= iota((TOK, TOK), 1))
    slot16 = iota((16, TOK), 0)
    row160 = iota((160, TOK), 0)
    row_slot = (jnp.where(row160 >= 80, row160 - 80, row160) >> 4) * 2 + ((row160 >> 2) & 1)
    for p in range(2):
        ranks = []
        for h in range(2):
            e = zlo if h == 0 else 1 - zlo
            match = ids[p] == e
            routed = jnp.max(jnp.where(match, 1.0, 0.0), axis=0, keepdims=True)
            w = jnp.sum(jnp.where(match, gates[p], 0.0), axis=0, keepdims=True)
            count = nn(jnp.broadcast_to(routed, (8, TOK)).astype(BF), upper)
            rank = jnp.where(routed > 0.5, count.astype(jnp.int32) - 1, -1)
            rk[p, h] = rank
            wts[p, h * 16:h * 16 + 16] = jnp.where(slot16 == rank[0:1], w, 0.0)
            ranks.append(rank[0:1])
        low = jnp.where(row_slot == ranks[0], 1.0, 0.0)
        high = jnp.where(row_slot == ranks[1], 1.0, 0.0)
        lhs[p] = jnp.where(row160 < 80, low, high).astype(BF)
    pl.semaphore_wait(barrier, len(peers))

    def extra(src, dst, k, dev):
        return pltpu.make_async_remote_copy(
            src_ref=src, dst_ref=dst, send_sem=xs.at[k], recv_sem=xr.at[k],
            device_id=dev, device_id_type=MESH,
        )

    wt_copies = [
        extra(wts.at[0], wt_out.at[0], WT0, {"section": nxt, "expert": exp}),
        extra(wts.at[1], wt_out.at[1], WT1, {"section": prv, "expert": exp}),
    ]
    for c in wt_copies:
        c.start()

    def weight(k, i):
        other = 1 - half
        if k == W_G:
            src, dst, dev = gw.at[0, feats(i, other), :], gu.at[i, :, pl.ds(FFD, FFD)], dev_p1
        elif k == W_U:
            src, dst, dev = uw.at[0, feats(i, other), :], gu.at[i, :, pl.ds(3 * FFD, FFD)], dev_p2
        elif k == W_DL:
            src = dw.at[0, pl.ds(64, 64), feats(i, other)]
            dst, dev = wd.at[i, pl.ds(192, 64), :], dev_ar
        else:
            src = dw.at[0, pl.ds(0, 64), feats(i, other)]
            dst, dev = wd.at[i, pl.ds(128, 64), :], dev_al
        return pltpu.make_async_remote_copy(
            src_ref=src, dst_ref=dst, send_sem=wss.at[k, i], recv_sem=wrs.at[k, i],
            device_id=dev, device_id_type=MESH,
        )

    for i in range(AHEAD):
        weight(W_G, i).start()
        weight(W_U, i).start()

    def ring(src, dst, k, j, dev):
        return pltpu.make_async_remote_copy(
            src_ref=src, dst_ref=dst,
            send_sem=ssem.at[0 if k < BO_L else 1, j], recv_sem=rsem.at[GROUP[k], j],
            device_id=dev, device_id_type=MESH,
        )

    def out(k, j):
        if k == Z:
            return ring(zbuf.at[j], zin.at[j], k, j, dev_z)
        if k == A_L:
            return ring(sbuf.at[j], gbuf.at[j, b, a], k, j, dev_ar)
        if k == A_R:
            return ring(sbuf.at[j], gbuf.at[j, b, a], k, j, dev_al)
        if k == A_O:
            return ring(gbuf.at[j, b, a], gbuf.at[j, b, a], k, j, dev_ao)
        if k == B_L:
            return ring(gbuf.at[j, b], gbuf.at[j, b], k, j, dev_br)
        if k == B_R:
            return ring(gbuf.at[j, b], gbuf.at[j, b], k, j, dev_bl)
        if k == FB_L:
            two = gbuf.at[j, bl, pl.ds(0, 2)]
            return ring(two, two, k, j, dev_br)
        if k == FB_R:
            two = gbuf.at[j, br, pl.ds(2, 2)]
            return ring(two, two, k, j, dev_bl)
        if k == BO_L:
            return ring(qbuf.at[j, bopp, pl.ds(0, 2)], bo.at[j, 0], k, j, dev_br)
        if k == BO_R:
            return ring(qbuf.at[j, bopp, pl.ds(2, 2)], bo.at[j, 1], k, j, dev_bl)
        if k == BN_L:
            return ring(qbuf.at[j, br], bn.at[j, 0], k, j, dev_br)
        if k == BN_R:
            return ring(qbuf.at[j, bl], bn.at[j, 1], k, j, dev_bl)
        if k == AN_L:
            return ring(qbuf.at[j, b, ar], an.at[j, 0], k, j, dev_ar)
        if k == AN_R:
            return ring(qbuf.at[j, b, al], an.at[j, 1], k, j, dev_al)
        if k == AN_O:
            return ring(qbuf.at[j, b, aopp], ao.at[j], k, j, dev_ao)
        to = jnp.where(j < NC, nxt, prv)
        h = k - FIN0
        dev = {"section": to, "expert": exp if h == 0 else partner}
        return ring(fbuf.at[j, h], fin.at[j, h], k, j, dev)

    def sized(n, sends, recvs):
        ref = size.at[pl.ds(0, n)]
        return pltpu.make_async_remote_copy(
            src_ref=ref, dst_ref=ref, send_sem=sends, recv_sem=recvs,
            device_id=dev_z, device_id_type=MESH,
        )

    def arrived(g, j):
        sized(BLOCKS[g], ssem.at[0, j], rsem.at[g, j]).wait_recv()

    def send(*kinds, j):
        for k in kinds:
            out(k, j).start()

    def sent(part, j):
        sized(SENT[part], ssem.at[part, j], rsem.at[0, j]).wait_send()

    def f32(v):
        return v.astype(F32)

    r16 = iota((SUB, FFD), 0)
    row_k = ((r16 >> 3) << 2) | (r16 & 3)

    def pack(j):
        p = j // NC
        load(act.at[0, :, pl.ds(0, CH)], tok.at[j], j).wait()
        y = nn(lhs[p], tok[j])
        for h in range(2):
            for c in range(5):
                r = (h * 5 + c) * SUB
                v = y[r:r + SUB, 0:FFD]
                for k in range(1, 8):
                    v = jnp.where(row_k == k, y[r:r + SUB, k * FFD:(k + 1) * FFD], v)
                if h == 0:
                    obuf[j, :, c * FFD:(c + 1) * FFD] = v.astype(BF)
                else:
                    zbuf[j, :, c * FFD:(c + 1) * FFD] = v.astype(BF)

    def by_half(j):
        o, z = f32(obuf[j]), f32(zin[j])
        first = jnp.concatenate([o[0:8], z[0:8]], axis=0)
        second = jnp.concatenate([o[8:16], z[8:16]], axis=0)
        gbuf[j, b, a] = jnp.where(half == 0, first, second).astype(BF)
        sbuf[j] = jnp.where(half == 0, second, first).astype(BF)

    def tables():
        o = iota((256, 256), 0)
        i = iota((256, 256), 1)
        perm_u[...] = onehot(i == ((o & 63) >> 2) * 16 + (o & 3) * 4 + (o >> 6))
        perm_p[...] = onehot(o == ((i & 63) >> 2) * 16 + (i & 3) * 4 + (i >> 6))
        o = iota((256, 160), 0)
        v = iota((256, 160), 1)
        h = jnp.where(v >= 80, 1, 0)
        slot = h * 16 + ((v - 80 * h) >> 4) * 2 + ((v >> 2) & 1)
        k = (((v >> 3) & 1) << 2) | (v & 3)
        sel[...] = onehot((k == (o >> 5)) & ((o & 31) == slot))

    def saved():
        for c in pres:
            c.wait()
        i = iota((ROWS, ROWS), 0)
        h = (i >> 1) & 1
        bp = (i >> 4) & 3
        ap = (i >> 2) & 3
        xy = ap * (4 - 3 * core) + bp * (1 + 3 * core)
        pln = zlo + h - 2 * zlo * h
        src = (pln * 16 + xy) * 10 + (i >> 6) * 2 + (i & 1)
        pref[...] = nn(onehot(iota((ROWS, ROWS), 1) == src), pre[...])

    def unpack(j):
        r = nn(perm_u[...], gbuf[j].reshape(256, PW)).astype(BF)
        for c in range(5):
            for k in range(4):
                xbuf[c * 64:(c + 1) * 64, k * FFD:(k + 1) * FFD] = (
                    r[k * 64:(k + 1) * 64, c * FFD:(c + 1) * FFD]
                )

    def repack(j, o):
        o = o.astype(BF)
        cols = []
        for c in range(5):
            cols.append(
                jnp.concatenate(
                    [o[c * 64:(c + 1) * 64, k * FFD:(k + 1) * FFD] for k in range(4)], axis=0
                )
            )
        q = nn(perm_p[...], jnp.concatenate(cols, axis=1)).astype(BF)
        qbuf[j] = q.reshape(4, 4, SUB, PW)

    def px_copies():
        return [
            extra(px.at[0], prx.at[0], PX_G, dev_p1),
            extra(px.at[1], prx.at[1], PX_U, dev_p2),
        ]

    def hid_copies():
        return [
            extra(hid, hx.at[0], HID_L, dev_ar),
            extra(hid, hx.at[1], HID_R, dev_al),
        ]

    def gh_copies():
        return [
            extra(ghx, ghr.at[0], GH_L, dev_ar),
            extra(ghx, ghr.at[1], GH_R, dev_al),
        ]

    def gg_copies():
        return [
            extra(gga.at[0], ggx.at[0], GG_G, dev_p1),
            extra(gga.at[1], ggx.at[1], GG_U, dev_p2),
        ]

    def forward_rows(i):
        own_weight(0, i).wait()
        own_weight(1, i).wait()
        weight(W_G, i).wait()
        weight(W_U, i).wait()

        @pl.when(i == 0)
        def _():
            acc[...] = nn(xbuf[...], gu[i])

        @pl.when(i > 0)
        def _():
            acc[...] += nn(xbuf[...], gu[i])

        @pl.when(i == NC - 1)
        def _():
            px[0] = acc[:, FFD:2 * FFD].astype(BF)
            px[1] = acc[:, 3 * FFD:4 * FFD].astype(BF)
            for c in px_copies():
                c.start()

    def backward_rows(i):
        own_weight(2, i).wait()
        weight(W_DL, i).wait()
        weight(W_DR, i).wait()

        @pl.when(i == 0)
        def _():
            accb[...] = nt(xbuf[...], wd[i])

        @pl.when(i > 0)
        def _():
            accb[...] += nt(xbuf[...], wd[i])

        @pl.when(i == NC - 1)
        def _():
            ghx[...] = accb[:, FFD:2 * FFD].astype(BF)
            for c in gh_copies():
                c.start()

    left64 = iota((ROWS, FFD), 1) < 64

    def hidden_own():
        for c in px_copies():
            c.wait()
        g = acc[:, 0:FFD] + f32(prx[0])
        u = acc[:, 2 * FFD:3 * FFD] + f32(prx[1])
        hid[...] = (g / (1.0 + jnp.exp(-g)) * u).astype(BF)
        for c in hid_copies():
            c.start()

    def hidden_all():
        for c in hid_copies():
            c.wait()
        hcat[:, 0:FFD] = hid[...]
        hcat[:, FFD:2 * FFD] = jnp.where(left64, f32(hx[1]), f32(hx[0])).astype(BF)

    def grads_own():
        for c in gh_copies():
            c.wait()
        gh = accb[:, 0:FFD] + jnp.where(left64, f32(ghr[0]), f32(ghr[1]))
        g = pref[:, 0:FFD]
        u = pref[:, FFD:2 * FFD]
        s = 1.0 / (1.0 + jnp.exp(-g))
        silu = g * s
        gga[0] = (gh * u * s * (1.0 + g * (1.0 - s))).astype(BF)
        gga[1] = (gh * silu).astype(BF)
        for c in gg_copies():
            c.start()
        dots = jnp.sum(gh * silu * u, axis=1, keepdims=True)
        at = iota((ROWS, FFD), 1) == (iota((ROWS, FFD), 0) >> 6)
        spot = jnp.where(at, jnp.broadcast_to(dots, (ROWS, FFD)), 0.0).astype(BF)
        o = iota((FFD, ROWS), 0)
        i2 = iota((FFD, ROWS), 1) & 63
        pick = onehot(((o & 7) < 4) & (i2 == (o >> 3) * 4 + (o & 7)))
        dbuf[...] = nn(pick, spot).reshape(4, 4, 8, FFD)

    def grads_all():
        for c in gg_copies():
            c.wait()
        ggu[:, 0:FFD] = gga[0]
        ggu[:, FFD:2 * FFD] = ggx[0]
        ggu[:, 2 * FFD:3 * FFD] = gga[1]
        ggu[:, 3 * FFD:4 * FFD] = ggx[1]

    @pl.loop(0, STEPS)
    def _(t):
        def event(lag, lo=0, hi=NJ):
            def wrap(f):
                @pl.when((t - lag >= lo) & (t - lag < hi))
                def _():
                    f(t - lag)
            return wrap

        @event(0)
        def _(j):
            pack(j)
            send(Z, j=j)

            @pl.when(j == 1)
            def _():
                tables()

        @event(E1)
        def _(j):
            arrived(GZ, j)
            by_half(j)
            send(A_L, A_R, A_O, j=j)

            @pl.when(j + AHEAD < NC)
            def _():
                weight(W_G, j + AHEAD).start()
                weight(W_U, j + AHEAD).start()

            @pl.when((j + AHEAD >= NC) & (j + AHEAD < NJ))
            def _():
                weight(W_DL, j + AHEAD - NC).start()
                weight(W_DR, j + AHEAD - NC).start()

        @event(E2)
        def _(j):
            arrived(GA, j)
            send(B_L, B_R, j=j)

        @event(E3)
        def _(j):
            arrived(GB, j)
            send(FB_L, FB_R, j=j)

        for step, act_now in ((X1, hidden_own), (X2, hidden_all), (X3, grads_own), (X4, grads_all)):
            pl.when(t == step)(act_now)

        @event(R0)
        def _(j):
            @pl.when(j < NC)
            def _():
                repack(j, nn(hcat[...], wd[j]))

            @pl.when(j >= NC)
            def _():
                repack(j, nt(ggu[...], gu[j - NC]))

            send(BO_L, BO_R, j=j)

            @pl.when(j == NC)
            def _():
                extra(dbuf.at[bopp], dbo, DBO, dev_br).start()

        @event(R1)
        def _(j):
            arrived(GBO, j)
            qbuf[j, br, 0:2] = (f32(qbuf[j, br, 0:2]) + f32(bo[j, 0])).astype(BF)
            qbuf[j, bl, 2:4] = (f32(qbuf[j, bl, 2:4]) + f32(bo[j, 1])).astype(BF)
            send(BN_L, BN_R, j=j)

            @pl.when(j == NC)
            def _():
                extra(dbuf.at[bopp], dbo, DBO, dev_br).wait()
                dbuf[br] = dbuf[br] + dbo[...]
                extra(dbuf.at[br], dbn.at[0], DBN_L, dev_br).start()
                extra(dbuf.at[bl], dbn.at[1], DBN_R, dev_bl).start()

        @event(R2)
        def _(j):
            arrived(GBN, j)
            qbuf[j, b] = (f32(qbuf[j, b]) + f32(bn[j, 0]) + f32(bn[j, 1])).astype(BF)
            send(AN_L, AN_R, AN_O, j=j)

            @pl.when(j == NC)
            def _():
                extra(dbuf.at[br], dbn.at[0], DBN_L, dev_br).wait()
                extra(dbuf.at[bl], dbn.at[1], DBN_R, dev_bl).wait()
                dbuf[b] = dbuf[b] + dbn[0] + dbn[1]
                extra(dbuf.at[b, aopp], dao, DAO, dev_ar).start()

        @event(R3)
        def _(j):
            arrived(GAN, j)
            mine = f32(qbuf[j, b, a]) + f32(ao[j])
            theirs = f32(an[j, 0]) + f32(an[j, 1])
            first = jnp.where(half == 0, mine, theirs)
            second = jnp.where(half == 0, theirs, mine)
            for h in range(2):
                r = h * 8
                fbuf[j, h] = jnp.concatenate([first[r:r + 8], second[r:r + 8]], axis=0).astype(BF)
            send(FIN0, FIN1, j=j)

            @pl.when(j == NC)
            def _():
                extra(dbuf.at[b, aopp], dao, DAO, dev_ar).wait()
                dbuf[b, ar] = dbuf[b, ar] + dao[...]
                extra(dbuf.at[b, ar], dan.at[0], DAN_L, dev_ar).start()
                extra(dbuf.at[b, al], dan.at[1], DAN_R, dev_al).start()

        @event(R4)
        def _(j):
            @pl.when(j == NC)
            def _():
                extra(dbuf.at[b, ar], dan.at[0], DAN_L, dev_ar).wait()
                extra(dbuf.at[b, al], dan.at[1], DAN_R, dev_al).wait()
                dfin[...] = dbuf[b, a] + dan[0] + dan[1]
                extra(dfin, dz, DZ, dev_z).start()

            arrived(GFIN, j)
            v = jnp.concatenate(
                [fin[j, h, :, c * FFD:(c + 1) * FFD] for h in range(2) for c in range(5)], axis=0
            )
            u = nn(sel[...], v).astype(BF)
            for k in range(8):
                ubuf[j, :, k * FFD:(k + 1) * FFD] = u[k * 32:(k + 1) * 32]
            pltpu.make_async_copy(ubuf.at[j], u_out.at[j], usem.at[j]).start()
            sent(1, j)

            @pl.when(j == NC + 2)
            def _():
                extra(dfin, dz, DZ, dev_z).wait()
                la = iota((8, FFD), 0)
                mine = jnp.where(la < 2, dfin[...], dz[...]).T
                c8 = iota((8, TOK), 0)
                which = ids[1]
                total = jnp.zeros((8, TOK), F32)
                for h in range(2):
                    d = jnp.zeros((8, TOK), F32)
                    for par in range(2):
                        hit = jnp.where((rk[1, h, 0:1] == c8 * 2 + par) & (c8 < 5), 1.0, 0.0)
                        d = d + hit * mine[0:8, h * 2 + par:h * 2 + par + 1]
                    d = jnp.sum(d, axis=0, keepdims=True)
                    e = zlo if h == 0 else 1 - zlo
                    total = total + jnp.where(which == e, d, 0.0)
                ggb[...] = total
                pltpu.make_async_copy(ggb, gg_out, osem).start()

        @event(E4)
        def _(j):
            @pl.when(j == 0)
            def _():
                saved()

            arrived(GFB, j)
            unpack(j)

            @pl.when(j < NC)
            def _():
                forward_rows(j)

            @pl.when(j >= NC)
            def _():
                backward_rows(j - NC)

            sent(0, j)

    for c in wt_copies:
        c.wait()
    pltpu.make_async_copy(ggb, gg_out, osem).wait()
    for j in range(NJ):
        pltpu.make_async_copy(ubuf.at[j], u_out.at[j], usem.at[j]).wait()


def relay(*args):
    any_spec = pl.BlockSpec(memory_space=pl.ANY)
    vmem = pltpu.VMEM
    dma = pltpu.SemaphoreType.DMA
    return pl.pallas_call(
        relay_kernel,
        out_shape=(
            jax.ShapeDtypeStruct((NJ, 32, CH), BF),
            jax.ShapeDtypeStruct((2, 32, TOK), F32),
            jax.ShapeDtypeStruct((8, TOK), F32),
        ),
        in_specs=[any_spec] * 11,
        out_specs=(any_spec,) * 3,
        scratch_shapes=[
            vmem((NJ, TOK, CH), BF),
            vmem((NC, HF, 4 * FFD), BF),
            vmem((NC, 2 * FFD, HF), BF),
            vmem((2, 8, TOK), jnp.int32),
            vmem((2, 8, TOK), F32),
            vmem((ROWS, 2 * FFD), BF),
            vmem((ROWS, 2 * FFD), F32),
            vmem((NJ, SUB, PW), BF),
            vmem((NJ, SUB, PW), BF),
            vmem((NJ, SUB, PW), BF),
            vmem((NJ, SUB, PW), BF),
            vmem((NJ, 4, 4, SUB, PW), BF),
            vmem((NJ, 4, 4, SUB, PW), BF),
            vmem((NJ, 2, 2, SUB, PW), BF),
            vmem((NJ, 2, 4, SUB, PW), BF),
            vmem((NJ, 2, SUB, PW), BF),
            vmem((NJ, SUB, PW), BF),
            vmem((NJ, 2, SUB, PW), BF),
            vmem((NJ, 2, SUB, PW), BF),
            vmem((NJ, 32, CH), BF),
            vmem((256, 160), BF),
            vmem((2, 160, TOK), BF),
            vmem((2, 2, 8, TOK), jnp.int32),
            vmem((2, 32, TOK), F32),
            vmem((256, 256), BF),
            vmem((256, 256), BF),
            vmem((ROWS, HF), BF),
            vmem((ROWS, 4 * FFD), F32),
            vmem((ROWS, 2 * FFD), F32),
            vmem((2, ROWS, FFD), BF),
            vmem((2, ROWS, FFD), BF),
            vmem((ROWS, FFD), BF),
            vmem((2, ROWS, FFD), BF),
            vmem((ROWS, 2 * FFD), BF),
            vmem((ROWS, FFD), BF),
            vmem((2, ROWS, FFD), BF),
            vmem((2, ROWS, FFD), BF),
            vmem((2, ROWS, FFD), BF),
            vmem((ROWS, 4 * FFD), BF),
            vmem((4, 4, 8, FFD), F32),
            vmem((4, 8, FFD), F32),
            vmem((2, 4, 8, FFD), F32),
            vmem((8, FFD), F32),
            vmem((2, 8, FFD), F32),
            vmem((8, FFD), F32),
            vmem((8, FFD), F32),
            vmem((8, TOK), F32),
            vmem((SENT[1], SUB, PW), BF),
            dma((2, NJ)),
            dma((NG, NJ)),
            dma((4, NC)),
            dma((4, NC)),
            dma((NX,)),
            dma((NX,)),
            dma((NJ + 6,)),
            dma((3, NC)),
            dma,
            dma((NJ,)),
        ],
        compiler_params=pltpu.CompilerParams(
            collective_id=0, has_side_effects=True, vmem_limit_bytes=62 * 2**20
        ),
        name="relay",
    )(*args)


def spread_kernel(u, wt, gg, next_ref, prev_ref, gg_ref, lhs, obuf, sems):
    gg_ref[0] = gg[...]
    for p in range(2):
        w = wt[p].T
        hi = w.astype(BF)
        lhs[p, :, 0:32] = hi
        lhs[p, :, 32:64] = (w - hi.astype(F32)).astype(BF)

    def copy(j):
        dst = next_ref if j < NC else prev_ref
        return pltpu.make_async_copy(
            obuf.at[j], dst.at[0, :, pl.ds((j % NC) * CH, CH)], sems.at[j]
        )

    for j in range(NJ):
        both = jnp.concatenate([u[j], u[j]], axis=0)
        obuf[j] = nn(lhs[j // NC], both).astype(BF)
        copy(j).start()
    for j in range(NJ):
        copy(j).wait()


def dense(u, wt, gg):
    vmem = pl.BlockSpec(memory_space=pltpu.VMEM)
    any_spec = pl.BlockSpec(memory_space=pl.ANY)
    return pl.pallas_call(
        spread_kernel,
        out_shape=(
            jax.ShapeDtypeStruct((1, TOK, D), BF),
            jax.ShapeDtypeStruct((1, TOK, D), BF),
            jax.ShapeDtypeStruct((1, 8, TOK), F32),
        ),
        in_specs=[vmem] * 3,
        out_specs=(any_spec, any_spec, vmem),
        scratch_shapes=[
            pltpu.VMEM((2, TOK, 64), BF),
            pltpu.VMEM((NJ, TOK, CH), BF),
            pltpu.SemaphoreType.DMA((NJ,)),
        ],
        compiler_params=pltpu.CompilerParams(vmem_limit_bytes=60 * 2**20),
        name="dense",
    )(u, wt, gg)


def body(*args):
    args = args[:2] + tuple(jnp.swapaxes(x, 1, 2) for x in args[2:6]) + args[6:]
    u, wt, gg = relay(*args)
    nxt, prv, grad = dense(u, wt, gg)
    return nxt, prv, jnp.swapaxes(grad, 1, 2)


def solution(mesh):
    rows = P("section", "expert", None)
    cols = P("section", None, "expert")
    return jax.shard_map(
        body,
        mesh=mesh,
        in_specs=(rows,) * 6 + (cols, cols, rows, cols, cols),
        out_specs=(rows,) * 3,
        check_vma=False,
    )
```

```python
import jax
import jax.numpy as jnp
from jax import lax
from jax.experimental import pallas as pl
from jax.experimental.pallas import tpu as pltpu
from jax.sharding import PartitionSpec as P

MESH = pl.DeviceIdType.MESH
BF = jnp.bfloat16
F32 = jnp.float32

D = 7168
NC = 7
CH = D // NC
NJ = 2 * NC
TOK = 128
FFD = 128
SUB = 16
PW = 640
ROWS = 320

(Z, A_L, A_R, A_O, B_L, B_R, FB_L, FB_R) = range(8)
(BO_L, BO_R, BN_L, BN_R, AN_L, AN_R, AN_O, FIN0, FIN1) = range(8, 17)
(GZ, GA, GB, GFB, GBO, GBN, GAN, GFIN) = range(8)
NG = 8
GROUP = (GZ, GA, GA, GA, GB, GB, GFB, GFB, GBO, GBO, GBN, GBN, GAN, GAN, GAN, GFIN, GFIN)
BLOCKS = (1, 3, 8, 4, 4, 8, 3, 2)
SENT = (16, 17)
(DBO, DBN_L, DBN_R, DAO, DAN_L, DAN_R, DZ, WT0, WT1) = range(9)
(PX_G, PX_U, HID_L, HID_R, GH_L, GH_R, GG_G, GG_U) = range(9, 17)
NX = 17
(W_G, W_U, W_DL, W_DR) = range(4)

AHEAD = 2
HF = CH // 2

E1, E2, E3, E4 = 1, 3, 5, 7
X1 = E4 + NC + 1
X2 = X1 + 2
R0 = E4 + 11
X3 = E4 + NJ + 1
X4 = X3 + 2
R1, R2, R3, R4 = R0 + 2, R0 + 5, R0 + 8, R0 + 11
STEPS = NJ + R4


def iota(shape, dim):
    return lax.broadcasted_iota(jnp.int32, shape, dim)


def onehot(cond):
    return jnp.where(cond, 1.0, 0.0).astype(BF)


def nn(a, b):
    return jnp.dot(a, b, preferred_element_type=F32)


def nt(a, b):
    return lax.dot_general(a, b, (((1,), (1,)), ((), ())), preferred_element_type=F32)


def relay_kernel(
    act, cot, fids, fgates, bids, bgates, gw, uw, dw, gpre, upre,
    u_out, wt_out, gg_out,
    tok, gu, wd, ids, gates, pre, pref, obuf, zbuf, zin, sbuf, gbuf,
    qbuf, bo, bn, an, ao, fbuf, fin, ubuf, sel,
    lhs, rk, wts, perm_u, perm_p, xbuf, acc, accb, px, prx, hid, hx, hcat, ghx, ghr, gga, ggx, ggu,
    dbuf, dbo, dbn, dao, dan, dfin, dz, ggb, size,
    ssem, rsem, wss, wrs, xs, xr, lsem, wsem, osem, usem,
):
    sec = lax.axis_index("section")
    exp = lax.axis_index("expert")
    core = lax.rem(sec, 2)
    zlo = exp // 16
    cx = lax.rem(exp // 4, 4)
    cy = lax.rem(exp, 4)
    a = cx * (1 - core) + cy * core
    b = cy * (1 - core) + cx * core
    half = lax.rem(a, 2)
    al, ar, aopp = lax.rem(a + 3, 4), lax.rem(a + 1, 4), lax.rem(a + 2, 4)
    bl, br, bopp = lax.rem(b + 3, 4), lax.rem(b + 1, 4), lax.rem(b + 2, 4)

    def plane(ap, bp):
        return zlo * 16 + ap * (4 - 3 * core) + bp * (1 + 3 * core)

    partner = exp + 16 - 32 * zlo
    dev_al, dev_ar = {"expert": plane(al, b)}, {"expert": plane(ar, b)}
    dev_ao = {"expert": plane(aopp, b)}
    dev_bl, dev_br = {"expert": plane(a, bl)}, {"expert": plane(a, br)}
    dev_p1 = {"expert": plane(a + 1 - 2 * half, b)}
    dev_p2 = {"expert": plane(lax.rem(a + 3 + 2 * half, 4), b)}
    dev_z = {"expert": partner}
    nxt, prv = lax.rem(sec + 1, 8), lax.rem(sec + 7, 8)

    def load(src, dst, k):
        return pltpu.make_async_copy(src, dst, lsem.at[k])

    small = [
        load(fids.at[0], ids.at[0], NJ),
        load(bids.at[0], ids.at[1], NJ + 1),
        load(fgates.at[0], gates.at[0], NJ + 2),
        load(bgates.at[0], gates.at[1], NJ + 3),
    ]
    pres = [
        load(gpre.at[0], pre.at[:, pl.ds(0, FFD)], NJ + 4),
        load(upre.at[0], pre.at[:, pl.ds(FFD, FFD)], NJ + 5),
    ]
    toks = []
    for j in range(NJ):
        src = act if j < NC else cot
        toks.append(load(src.at[0, :, pl.ds((j % NC) * CH, CH)], tok.at[j], j))

    def feats(i, h):
        return pl.ds(pl.multiple_of(i * CH + h * HF, HF), HF)

    def own_weight(k, i):
        src = (gw, uw, dw)[k]
        if k < 2:
            src = src.at[0, feats(i, half), :]
            dst = gu.at[i, :, pl.ds(2 * k * FFD, FFD)]
        else:
            src = src.at[0, :, feats(i, half)]
            dst = wd.at[i, pl.ds(0, FFD), :]
        return pltpu.make_async_copy(src, dst, wsem.at[k, i])

    for c in small:
        c.start()
    for c in toks[:NC]:
        c.start()
    for i in range(NC):
        own_weight(0, i).start()
        own_weight(1, i).start()
    for c in toks[NC:]:
        c.start()
    for i in range(NC):
        own_weight(2, i).start()
    for c in pres:
        c.start()

    barrier = pltpu.get_barrier_semaphore()
    peers = [dev_al, dev_ar, dev_ao, dev_bl, dev_br, dev_z]
    for s in (nxt, prv):
        peers.append({"section": s, "expert": exp})
        peers.append({"section": s, "expert": partner})
    for dev in peers:
        pl.semaphore_signal(barrier, inc=1, device_id=dev, device_id_type=MESH)

    for c in small:
        c.wait()
    upper = onehot(iota((TOK, TOK), 0) <= iota((TOK, TOK), 1))
    slot16 = iota((16, TOK), 0)
    row160 = iota((160, TOK), 0)
    row_slot = (jnp.where(row160 >= 80, row160 - 80, row160) >> 4) * 2 + ((row160 >> 2) & 1)
    for p in range(2):
        ranks = []
        for h in range(2):
            e = zlo if h == 0 else 1 - zlo
            match = ids[p] == e
            routed = jnp.max(jnp.where(match, 1.0, 0.0), axis=0, keepdims=True)
            w = jnp.sum(jnp.where(match, gates[p], 0.0), axis=0, keepdims=True)
            count = nn(jnp.broadcast_to(routed, (8, TOK)).astype(BF), upper)
            rank = jnp.where(routed > 0.5, count.astype(jnp.int32) - 1, -1)
            rk[p, h] = rank
            wts[p, h * 16:h * 16 + 16] = jnp.where(slot16 == rank[0:1], w, 0.0)
            ranks.append(rank[0:1])
        low = jnp.where(row_slot == ranks[0], 1.0, 0.0)
        high = jnp.where(row_slot == ranks[1], 1.0, 0.0)
        lhs[p] = jnp.where(row160 < 80, low, high).astype(BF)
    pl.semaphore_wait(barrier, len(peers))

    def extra(src, dst, k, dev):
        return pltpu.make_async_remote_copy(
            src_ref=src, dst_ref=dst, send_sem=xs.at[k], recv_sem=xr.at[k],
            device_id=dev, device_id_type=MESH,
        )

    wt_copies = [
        extra(wts.at[0], wt_out.at[0], WT0, {"section": nxt, "expert": exp}),
        extra(wts.at[1], wt_out.at[1], WT1, {"section": prv, "expert": exp}),
    ]
    for c in wt_copies:
        c.start()

    def weight(k, i):
        other = 1 - half
        if k == W_G:
            src, dst, dev = gw.at[0, feats(i, other), :], gu.at[i, :, pl.ds(FFD, FFD)], dev_p1
        elif k == W_U:
            src, dst, dev = uw.at[0, feats(i, other), :], gu.at[i, :, pl.ds(3 * FFD, FFD)], dev_p2
        elif k == W_DL:
            src = dw.at[0, pl.ds(64, 64), feats(i, other)]
            dst, dev = wd.at[i, pl.ds(192, 64), :], dev_ar
        else:
            src = dw.at[0, pl.ds(0, 64), feats(i, other)]
            dst, dev = wd.at[i, pl.ds(128, 64), :], dev_al
        return pltpu.make_async_remote_copy(
            src_ref=src, dst_ref=dst, send_sem=wss.at[k, i], recv_sem=wrs.at[k, i],
            device_id=dev, device_id_type=MESH,
        )

    for i in range(AHEAD):
        weight(W_G, i).start()
        weight(W_U, i).start()

    def ring(src, dst, k, j, dev):
        return pltpu.make_async_remote_copy(
            src_ref=src, dst_ref=dst,
            send_sem=ssem.at[0 if k < BO_L else 1, j], recv_sem=rsem.at[GROUP[k], j],
            device_id=dev, device_id_type=MESH,
        )

    def out(k, j):
        if k == Z:
            return ring(zbuf.at[j], zin.at[j], k, j, dev_z)
        if k == A_L:
            return ring(sbuf.at[j], gbuf.at[j, b, a], k, j, dev_ar)
        if k == A_R:
            return ring(sbuf.at[j], gbuf.at[j, b, a], k, j, dev_al)
        if k == A_O:
            return ring(gbuf.at[j, b, a], gbuf.at[j, b, a], k, j, dev_ao)
        if k == B_L:
            return ring(gbuf.at[j, b], gbuf.at[j, b], k, j, dev_br)
        if k == B_R:
            return ring(gbuf.at[j, b], gbuf.at[j, b], k, j, dev_bl)
        if k == FB_L:
            two = gbuf.at[j, bl, pl.ds(0, 2)]
            return ring(two, two, k, j, dev_br)
        if k == FB_R:
            two = gbuf.at[j, br, pl.ds(2, 2)]
            return ring(two, two, k, j, dev_bl)
        if k == BO_L:
            return ring(qbuf.at[j, bopp, pl.ds(0, 2)], bo.at[j, 0], k, j, dev_br)
        if k == BO_R:
            return ring(qbuf.at[j, bopp, pl.ds(2, 2)], bo.at[j, 1], k, j, dev_bl)
        if k == BN_L:
            return ring(qbuf.at[j, br], bn.at[j, 0], k, j, dev_br)
        if k == BN_R:
            return ring(qbuf.at[j, bl], bn.at[j, 1], k, j, dev_bl)
        if k == AN_L:
            return ring(qbuf.at[j, b, ar], an.at[j, 0], k, j, dev_ar)
        if k == AN_R:
            return ring(qbuf.at[j, b, al], an.at[j, 1], k, j, dev_al)
        if k == AN_O:
            return ring(qbuf.at[j, b, aopp], ao.at[j], k, j, dev_ao)
        to = jnp.where(j < NC, nxt, prv)
        h = k - FIN0
        dev = {"section": to, "expert": exp if h == 0 else partner}
        return ring(fbuf.at[j, h], fin.at[j, h], k, j, dev)

    def sized(n, sends, recvs):
        ref = size.at[pl.ds(0, n)]
        return pltpu.make_async_remote_copy(
            src_ref=ref, dst_ref=ref, send_sem=sends, recv_sem=recvs,
            device_id=dev_z, device_id_type=MESH,
        )

    def arrived(g, j):
        sized(BLOCKS[g], ssem.at[0, j], rsem.at[g, j]).wait_recv()

    def send(*kinds, j):
        for k in kinds:
            out(k, j).start()

    def sent(part, j):
        sized(SENT[part], ssem.at[part, j], rsem.at[0, j]).wait_send()

    def f32(v):
        return v.astype(F32)

    r16 = iota((SUB, FFD), 0)
    row_k = ((r16 >> 3) << 2) | (r16 & 3)

    def pack(j):
        p = j // NC
        load(act.at[0, :, pl.ds(0, CH)], tok.at[j], j).wait()
        y = nn(lhs[p], tok[j])
        for h in range(2):
            for c in range(5):
                r = (h * 5 + c) * SUB
                v = y[r:r + SUB, 0:FFD]
                for k in range(1, 8):
                    v = jnp.where(row_k == k, y[r:r + SUB, k * FFD:(k + 1) * FFD], v)
                if h == 0:
                    obuf[j, :, c * FFD:(c + 1) * FFD] = v.astype(BF)
                else:
                    zbuf[j, :, c * FFD:(c + 1) * FFD] = v.astype(BF)

    def by_half(j):
        o, z = f32(obuf[j]), f32(zin[j])
        first = jnp.concatenate([o[0:8], z[0:8]], axis=0)
        second = jnp.concatenate([o[8:16], z[8:16]], axis=0)
        gbuf[j, b, a] = jnp.where(half == 0, first, second).astype(BF)
        sbuf[j] = jnp.where(half == 0, second, first).astype(BF)

    def tables():
        o = iota((256, 256), 0)
        i = iota((256, 256), 1)
        perm_u[...] = onehot(i == ((o & 63) >> 2) * 16 + (o & 3) * 4 + (o >> 6))
        perm_p[...] = onehot(o == ((i & 63) >> 2) * 16 + (i & 3) * 4 + (i >> 6))
        o = iota((256, 160), 0)
        v = iota((256, 160), 1)
        h = jnp.where(v >= 80, 1, 0)
        slot = h * 16 + ((v - 80 * h) >> 4) * 2 + ((v >> 2) & 1)
        k = (((v >> 3) & 1) << 2) | (v & 3)
        sel[...] = onehot((k == (o >> 5)) & ((o & 31) == slot))

    def saved():
        for c in pres:
            c.wait()
        i = iota((ROWS, ROWS), 0)
        h = (i >> 1) & 1
        bp = (i >> 4) & 3
        ap = (i >> 2) & 3
        xy = ap * (4 - 3 * core) + bp * (1 + 3 * core)
        pln = zlo + h - 2 * zlo * h
        src = (pln * 16 + xy) * 10 + (i >> 6) * 2 + (i & 1)
        pref[...] = nn(onehot(iota((ROWS, ROWS), 1) == src), pre[...])

    def unpack(j):
        r = nn(perm_u[...], gbuf[j].reshape(256, PW)).astype(BF)
        for c in range(5):
            for k in range(4):
                xbuf[c * 64:(c + 1) * 64, k * FFD:(k + 1) * FFD] = (
                    r[k * 64:(k + 1) * 64, c * FFD:(c + 1) * FFD]
                )

    def repack(j, o):
        o = o.astype(BF)
        cols = []
        for c in range(5):
            cols.append(
                jnp.concatenate(
                    [o[c * 64:(c + 1) * 64, k * FFD:(k + 1) * FFD] for k in range(4)], axis=0
                )
            )
        q = nn(perm_p[...], jnp.concatenate(cols, axis=1)).astype(BF)
        qbuf[j] = q.reshape(4, 4, SUB, PW)

    def px_copies():
        return [
            extra(px.at[0], prx.at[0], PX_G, dev_p1),
            extra(px.at[1], prx.at[1], PX_U, dev_p2),
        ]

    def hid_copies():
        return [
            extra(hid, hx.at[0], HID_L, dev_ar),
            extra(hid, hx.at[1], HID_R, dev_al),
        ]

    def gh_copies():
        return [
            extra(ghx, ghr.at[0], GH_L, dev_ar),
            extra(ghx, ghr.at[1], GH_R, dev_al),
        ]

    def gg_copies():
        return [
            extra(gga.at[0], ggx.at[0], GG_G, dev_p1),
            extra(gga.at[1], ggx.at[1], GG_U, dev_p2),
        ]

    def forward_rows(i):
        own_weight(0, i).wait()
        own_weight(1, i).wait()
        weight(W_G, i).wait()
        weight(W_U, i).wait()

        @pl.when(i == 0)
        def _():
            acc[...] = nn(xbuf[...], gu[i])

        @pl.when(i > 0)
        def _():
            acc[...] += nn(xbuf[...], gu[i])

        @pl.when(i == NC - 1)
        def _():
            px[0] = acc[:, FFD:2 * FFD].astype(BF)
            px[1] = acc[:, 3 * FFD:4 * FFD].astype(BF)
            for c in px_copies():
                c.start()

    def backward_rows(i):
        own_weight(2, i).wait()
        weight(W_DL, i).wait()
        weight(W_DR, i).wait()

        @pl.when(i == 0)
        def _():
            accb[...] = nt(xbuf[...], wd[i])

        @pl.when(i > 0)
        def _():
            accb[...] += nt(xbuf[...], wd[i])

        @pl.when(i == NC - 1)
        def _():
            ghx[...] = accb[:, FFD:2 * FFD].astype(BF)
            for c in gh_copies():
                c.start()

    left64 = iota((ROWS, FFD), 1) < 64

    def hidden_own():
        for c in px_copies():
            c.wait()
        g = acc[:, 0:FFD] + f32(prx[0])
        u = acc[:, 2 * FFD:3 * FFD] + f32(prx[1])
        hid[...] = (g / (1.0 + jnp.exp(-g)) * u).astype(BF)
        for c in hid_copies():
            c.start()

    def hidden_all():
        for c in hid_copies():
            c.wait()
        hcat[:, 0:FFD] = hid[...]
        hcat[:, FFD:2 * FFD] = jnp.where(left64, f32(hx[1]), f32(hx[0])).astype(BF)

    def grads_own():
        for c in gh_copies():
            c.wait()
        gh = accb[:, 0:FFD] + jnp.where(left64, f32(ghr[0]), f32(ghr[1]))
        g = pref[:, 0:FFD]
        u = pref[:, FFD:2 * FFD]
        s = 1.0 / (1.0 + jnp.exp(-g))
        silu = g * s
        gga[0] = (gh * u * s * (1.0 + g * (1.0 - s))).astype(BF)
        gga[1] = (gh * silu).astype(BF)
        for c in gg_copies():
            c.start()
        dots = jnp.sum(gh * silu * u, axis=1, keepdims=True)
        at = iota((ROWS, FFD), 1) == (iota((ROWS, FFD), 0) >> 6)
        spot = jnp.where(at, jnp.broadcast_to(dots, (ROWS, FFD)), 0.0).astype(BF)
        o = iota((FFD, ROWS), 0)
        i2 = iota((FFD, ROWS), 1) & 63
        pick = onehot(((o & 7) < 4) & (i2 == (o >> 3) * 4 + (o & 7)))
        dbuf[...] = nn(pick, spot).reshape(4, 4, 8, FFD)

    def grads_all():
        for c in gg_copies():
            c.wait()
        ggu[:, 0:FFD] = gga[0]
        ggu[:, FFD:2 * FFD] = ggx[0]
        ggu[:, 2 * FFD:3 * FFD] = gga[1]
        ggu[:, 3 * FFD:4 * FFD] = ggx[1]

    @pl.loop(0, STEPS)
    def _(t):
        def event(lag, lo=0, hi=NJ):
            def wrap(f):
                @pl.when((t - lag >= lo) & (t - lag < hi))
                def _():
                    f(t - lag)
            return wrap

        @event(R0)
        def _(j):
            @pl.when(j < NC)
            def _():
                repack(j, nn(hcat[...], wd[j]))

            @pl.when(j >= NC)
            def _():
                repack(j, nt(ggu[...], gu[j - NC]))

            send(BO_L, BO_R, j=j)

            @pl.when(j == NC)
            def _():
                extra(dbuf.at[bopp], dbo, DBO, dev_br).start()

        @event(0)
        def _(j):
            pack(j)
            send(Z, j=j)

            @pl.when(j == 1)
            def _():
                tables()

        @event(E1)
        def _(j):
            arrived(GZ, j)
            by_half(j)
            send(A_L, A_R, A_O, j=j)

            @pl.when(j + AHEAD < NC)
            def _():
                weight(W_G, j + AHEAD).start()
                weight(W_U, j + AHEAD).start()

            @pl.when((j + AHEAD >= NC) & (j + AHEAD < NJ))
            def _():
                weight(W_DL, j + AHEAD - NC).start()
                weight(W_DR, j + AHEAD - NC).start()

        @event(E2)
        def _(j):
            arrived(GA, j)
            send(B_L, B_R, j=j)

        @event(E3)
        def _(j):
            arrived(GB, j)
            send(FB_L, FB_R, j=j)

        for step, act_now in ((X1, hidden_own), (X2, hidden_all), (X3, grads_own), (X4, grads_all)):
            pl.when(t == step)(act_now)

        @event(R1)
        def _(j):
            arrived(GBO, j)
            qbuf[j, br, 0:2] = (f32(qbuf[j, br, 0:2]) + f32(bo[j, 0])).astype(BF)
            qbuf[j, bl, 2:4] = (f32(qbuf[j, bl, 2:4]) + f32(bo[j, 1])).astype(BF)
            send(BN_L, BN_R, j=j)

            @pl.when(j == NC)
            def _():
                extra(dbuf.at[bopp], dbo, DBO, dev_br).wait()
                dbuf[br] = dbuf[br] + dbo[...]
                extra(dbuf.at[br], dbn.at[0], DBN_L, dev_br).start()
                extra(dbuf.at[bl], dbn.at[1], DBN_R, dev_bl).start()

        @event(R2)
        def _(j):
            arrived(GBN, j)
            qbuf[j, b] = (f32(qbuf[j, b]) + f32(bn[j, 0]) + f32(bn[j, 1])).astype(BF)
            send(AN_L, AN_R, AN_O, j=j)

            @pl.when(j == NC)
            def _():
                extra(dbuf.at[br], dbn.at[0], DBN_L, dev_br).wait()
                extra(dbuf.at[bl], dbn.at[1], DBN_R, dev_bl).wait()
                dbuf[b] = dbuf[b] + dbn[0] + dbn[1]
                extra(dbuf.at[b, aopp], dao, DAO, dev_ar).start()

        @event(R3)
        def _(j):
            arrived(GAN, j)
            mine = f32(qbuf[j, b, a]) + f32(ao[j])
            theirs = f32(an[j, 0]) + f32(an[j, 1])
            first = jnp.where(half == 0, mine, theirs)
            second = jnp.where(half == 0, theirs, mine)
            for h in range(2):
                r = h * 8
                fbuf[j, h] = jnp.concatenate([first[r:r + 8], second[r:r + 8]], axis=0).astype(BF)
            send(FIN0, FIN1, j=j)

            @pl.when(j == NC)
            def _():
                extra(dbuf.at[b, aopp], dao, DAO, dev_ar).wait()
                dbuf[b, ar] = dbuf[b, ar] + dao[...]
                extra(dbuf.at[b, ar], dan.at[0], DAN_L, dev_ar).start()
                extra(dbuf.at[b, al], dan.at[1], DAN_R, dev_al).start()

        @event(R4)
        def _(j):
            @pl.when(j == NC)
            def _():
                extra(dbuf.at[b, ar], dan.at[0], DAN_L, dev_ar).wait()
                extra(dbuf.at[b, al], dan.at[1], DAN_R, dev_al).wait()
                dfin[...] = dbuf[b, a] + dan[0] + dan[1]
                extra(dfin, dz, DZ, dev_z).start()

            arrived(GFIN, j)
            v = jnp.concatenate(
                [fin[j, h, :, c * FFD:(c + 1) * FFD] for h in range(2) for c in range(5)], axis=0
            )
            u = nn(sel[...], v).astype(BF)
            for k in range(8):
                ubuf[j, :, k * FFD:(k + 1) * FFD] = u[k * 32:(k + 1) * 32]
            pltpu.make_async_copy(ubuf.at[j], u_out.at[j], usem.at[j]).start()
            sent(1, j)

            @pl.when(j == NC + 2)
            def _():
                extra(dfin, dz, DZ, dev_z).wait()
                la = iota((8, FFD), 0)
                mine = jnp.where(la < 2, dfin[...], dz[...]).T
                c8 = iota((8, TOK), 0)
                which = ids[1]
                total = jnp.zeros((8, TOK), F32)
                for h in range(2):
                    d = jnp.zeros((8, TOK), F32)
                    for par in range(2):
                        hit = jnp.where((rk[1, h, 0:1] == c8 * 2 + par) & (c8 < 5), 1.0, 0.0)
                        d = d + hit * mine[0:8, h * 2 + par:h * 2 + par + 1]
                    d = jnp.sum(d, axis=0, keepdims=True)
                    e = zlo if h == 0 else 1 - zlo
                    total = total + jnp.where(which == e, d, 0.0)
                ggb[...] = total
                pltpu.make_async_copy(ggb, gg_out, osem).start()

        @event(E4)
        def _(j):
            @pl.when(j == 0)
            def _():
                saved()

            arrived(GFB, j)
            unpack(j)

            @pl.when(j < NC)
            def _():
                forward_rows(j)

            @pl.when(j >= NC)
            def _():
                backward_rows(j - NC)

            sent(0, j)

    for c in wt_copies:
        c.wait()
    pltpu.make_async_copy(ggb, gg_out, osem).wait()
    for j in range(NJ):
        pltpu.make_async_copy(ubuf.at[j], u_out.at[j], usem.at[j]).wait()


def relay(*args):
    any_spec = pl.BlockSpec(memory_space=pl.ANY)
    vmem = pltpu.VMEM
    dma = pltpu.SemaphoreType.DMA
    return pl.pallas_call(
        relay_kernel,
        out_shape=(
            jax.ShapeDtypeStruct((NJ, 32, CH), BF),
            jax.ShapeDtypeStruct((2, 32, TOK), F32),
            jax.ShapeDtypeStruct((8, TOK), F32),
        ),
        in_specs=[any_spec] * 11,
        out_specs=(any_spec,) * 3,
        scratch_shapes=[
            vmem((NJ, TOK, CH), BF),
            vmem((NC, HF, 4 * FFD), BF),
            vmem((NC, 2 * FFD, HF), BF),
            vmem((2, 8, TOK), jnp.int32),
            vmem((2, 8, TOK), F32),
            vmem((ROWS, 2 * FFD), BF),
            vmem((ROWS, 2 * FFD), F32),
            vmem((NJ, SUB, PW), BF),
            vmem((NJ, SUB, PW), BF),
            vmem((NJ, SUB, PW), BF),
            vmem((NJ, SUB, PW), BF),
            vmem((NJ, 4, 4, SUB, PW), BF),
            vmem((NJ, 4, 4, SUB, PW), BF),
            vmem((NJ, 2, 2, SUB, PW), BF),
            vmem((NJ, 2, 4, SUB, PW), BF),
            vmem((NJ, 2, SUB, PW), BF),
            vmem((NJ, SUB, PW), BF),
            vmem((NJ, 2, SUB, PW), BF),
            vmem((NJ, 2, SUB, PW), BF),
            vmem((NJ, 32, CH), BF),
            vmem((256, 160), BF),
            vmem((2, 160, TOK), BF),
            vmem((2, 2, 8, TOK), jnp.int32),
            vmem((2, 32, TOK), F32),
            vmem((256, 256), BF),
            vmem((256, 256), BF),
            vmem((ROWS, HF), BF),
            vmem((ROWS, 4 * FFD), F32),
            vmem((ROWS, 2 * FFD), F32),
            vmem((2, ROWS, FFD), BF),
            vmem((2, ROWS, FFD), BF),
            vmem((ROWS, FFD), BF),
            vmem((2, ROWS, FFD), BF),
            vmem((ROWS, 2 * FFD), BF),
            vmem((ROWS, FFD), BF),
            vmem((2, ROWS, FFD), BF),
            vmem((2, ROWS, FFD), BF),
            vmem((2, ROWS, FFD), BF),
            vmem((ROWS, 4 * FFD), BF),
            vmem((4, 4, 8, FFD), F32),
            vmem((4, 8, FFD), F32),
            vmem((2, 4, 8, FFD), F32),
            vmem((8, FFD), F32),
            vmem((2, 8, FFD), F32),
            vmem((8, FFD), F32),
            vmem((8, FFD), F32),
            vmem((8, TOK), F32),
            vmem((SENT[1], SUB, PW), BF),
            dma((2, NJ)),
            dma((NG, NJ)),
            dma((4, NC)),
            dma((4, NC)),
            dma((NX,)),
            dma((NX,)),
            dma((NJ + 6,)),
            dma((3, NC)),
            dma,
            dma((NJ,)),
        ],
        compiler_params=pltpu.CompilerParams(
            collective_id=0, has_side_effects=True, vmem_limit_bytes=62 * 2**20
        ),
        name="relay",
    )(*args)


def spread_kernel(u, wt, gg, next_ref, prev_ref, gg_ref, lhs, obuf, sems):
    gg_ref[0] = gg[...]
    for p in range(2):
        w = wt[p].T
        hi = w.astype(BF)
        lhs[p, :, 0:32] = hi
        lhs[p, :, 32:64] = (w - hi.astype(F32)).astype(BF)

    def copy(j):
        dst = next_ref if j < NC else prev_ref
        return pltpu.make_async_copy(
            obuf.at[j], dst.at[0, :, pl.ds((j % NC) * CH, CH)], sems.at[j]
        )

    for j in range(NJ):
        both = jnp.concatenate([u[j], u[j]], axis=0)
        obuf[j] = nn(lhs[j // NC], both).astype(BF)
        copy(j).start()
    for j in range(NJ):
        copy(j).wait()


def dense(u, wt, gg):
    vmem = pl.BlockSpec(memory_space=pltpu.VMEM)
    any_spec = pl.BlockSpec(memory_space=pl.ANY)
    return pl.pallas_call(
        spread_kernel,
        out_shape=(
            jax.ShapeDtypeStruct((1, TOK, D), BF),
            jax.ShapeDtypeStruct((1, TOK, D), BF),
            jax.ShapeDtypeStruct((1, 8, TOK), F32),
        ),
        in_specs=[vmem] * 3,
        out_specs=(any_spec, any_spec, vmem),
        scratch_shapes=[
            pltpu.VMEM((2, TOK, 64), BF),
            pltpu.VMEM((NJ, TOK, CH), BF),
            pltpu.SemaphoreType.DMA((NJ,)),
        ],
        compiler_params=pltpu.CompilerParams(vmem_limit_bytes=60 * 2**20),
        name="dense",
    )(u, wt, gg)


def body(*args):
    args = args[:2] + tuple(jnp.swapaxes(x, 1, 2) for x in args[2:6]) + args[6:]
    u, wt, gg = relay(*args)
    nxt, prv, grad = dense(u, wt, gg)
    return nxt, prv, jnp.swapaxes(grad, 1, 2)


def solution(mesh):
    rows = P("section", "expert", None)
    cols = P("section", None, "expert")
    return jax.shard_map(
        body,
        mesh=mesh,
        in_specs=(rows,) * 6 + (cols, cols, rows, cols, cols),
        out_specs=(rows,) * 3,
        check_vma=False,
    )
```
